256 devices in a mesh: expert: 8 (over x, core), ffn: 32 (over z, y).
Axes of the slice: x: 4, y: 4, z: 8, core: 2. Of those that a mesh axis runs over, the one named last changes fastest.
Arguments:
- tokens: bfloat16 [8, 128, 4096], P('expert', 'ffn'), may hold values from -6 to 6
- routes: int32 [8, 128, 2], P('expert'), may hold values from 0 to 7, all different within a row; in each aligned block of 128 rows (0 to 127, 128 to 255, ..., all dimensions but the last counted through in order) at most 48 rows name the same one
- router: bfloat16 [4096, 8], replicated, may hold values from -0.09375 to 0.09375
- w_gate: bfloat16 [8, 4096, 12288], P('expert', None, 'ffn'), may hold values from -0.09375 to 0.09375
- w_up: bfloat16 [8, 4096, 12288], P('expert', None, 'ffn'), may hold values from -0.09375 to 0.09375
- w_down: bfloat16 [8, 12288, 4096], P('expert', 'ffn'), may hold values from -0.109375 to 0.109375
- adapter: bfloat16 [8, 4096, 4096], P('expert', None, 'ffn'), may hold values from -0.09375 to 0.09375
- upstream: bfloat16 [8, 128, 4096], P('expert', None, 'ffn'), may hold values from -24 to 24
- bound: float32 [8], P('expert'), may hold values from 2048 to 16384
Outputs:
- adapted: bfloat16 [8, 128, 4096], P('expert', None, 'ffn')
- clipped: bfloat16 [8, 4096, 4096], P('expert', None, 'ffn')
The draws below stay inside these ranges and needn't reach their ends.
Inputs may be any that keep to these rules, and one draw needn't show every extreme that they name: `routes`: each token names two different experts; for each client at most 48 of its tokens name any one expert, and in some clients some expert is named by exactly 48 tokens.
All inputs are finite; a program needn't handle non-finite values.
Results may differ from the reference program's by a relative error of at most 0.015.
Values may be sent and summed in bfloat16 or wider, within the bound.
A program may use at most 64 MiB of HBM per device.

```python
import math
import jax
import jax.numpy as jnp
import numpy as np
from jax import lax

D = 4096
FF = 12288
EXPERTS = 8
CLIENTS = 8
TOK_CL = 128
CAP = 48
FF_DEV = 384
COLS_DEV = 128
N_FFN = 32


def draw_upstream(key, part):
    key_noise = jax.random.fold_in(key, 11)
    key_scale = jax.random.fold_in(key, 23)
    noise_part = jax.random.normal(key_noise, (CLIENTS, TOK_CL, D), jnp.float32)
    block_scales = jnp.exp(jax.random.uniform(key_scale, (CLIENTS, 1, D // COLS_DEV), jnp.float32, math.log(0.25), math.log(4.0)))
    scales = jnp.repeat(block_scales, COLS_DEV, axis=2)
    values = noise_part * scales
    return jnp.clip(values, -24.0, 24.0).astype(jnp.bfloat16)


def raised(array, own_key, source, target, blocks, factor):
    def block_of(position):
        return (jnp.arange(array.shape[position]) // (array.shape[position] // blocks)).reshape((-1,) + (1,) * (array.ndim - 1 - position))

    first = jax.random.permutation(own_key, blocks)[block_of(target)]
    far = (block_of(target) + blocks // 2) % blocks
    return jnp.where((block_of(source) == first) | (block_of(source) == far), factor * array, array)


def shard_levels(key, extent, cuts, smallest, largest):
    loudness = 1.0
    for position, parts in cuts:
        steps = jax.random.uniform(jax.random.fold_in(jax.random.fold_in(key, 6), position), (parts,), jnp.float32, smallest / len(cuts), largest / len(cuts))
        loudness = loudness * jnp.repeat(jnp.exp(steps), extent[position] // parts).reshape((-1,) + (1,) * (len(extent) - 1 - position))
    return loudness


def routed_block(key, own, number, rows, number_of, top, limit, lean):
    sequence = jax.random.permutation(key, number_of)
    crowded, ordinary = shares(number_of, rows * top, limit, lean, True), shares(number_of, rows * top, limit, lean, False)
    places = jnp.arange(number_of)

    def named(tallies, turn):
        used = int((tallies > 0).sum())
        fixed = max(1, used // 4)
        passed = fixed + (places - fixed + turn * (used - fixed)) % max(1, number_of - fixed)
        return jnp.zeros((number_of,), jnp.int32).at[sequence[jnp.where(places < fixed, places, passed)]].set(jnp.asarray(tallies, jnp.int32))

    tallies = jnp.where(number % 4 == 0, named(crowded, number // 4), named(ordinary, number - number // 4 - 1))
    mixed = jax.random.permutation(jax.random.fold_in(own, 3), number_of)
    donor, taker = mixed[0:number_of // 2 * 2:2], mixed[1:number_of // 2 * 2:2]
    slack = jnp.minimum(tallies[donor] - 1, limit - tallies[taker]) // 2
    slack = jnp.where((donor == sequence[0]) | (taker == sequence[0]) | (tallies[taker] == 0), 0, jnp.maximum(slack, 0))
    passed = jax.random.randint(jax.random.fold_in(own, 4), (number_of // 2,), 0, 1 << 20) % (slack + 1)
    tallies = tallies.at[donor].add(-passed).at[taker].add(passed)
    members = jnp.searchsorted(jnp.cumsum(tallies), jnp.arange(rows * top), side="right").astype(jnp.int32)
    grid = members.reshape(top, rows).T
    grid = grid[jax.random.permutation(jax.random.fold_in(own, 1), rows)]
    turn = jax.random.randint(jax.random.fold_in(own, 2), (rows, 1), 0, top)
    return jnp.take_along_axis(grid, (jnp.arange(top)[None, :] + turn) % top, axis=1)


def shares(amount, total, most, skew, full):
    loads = [(1 << 20) // math.isqrt(grade ** skew) + 1 for grade in range(1, amount + 1)]
    largest = most if full else min(most, max(-(-total // amount), total * loads[0] // sum(loads)))
    least = 1 if total - largest >= amount - 1 else 0
    counts, spare = [largest] + [least] * (amount - 1), total - largest - least * (amount - 1)
    while spare > 0:
        candidates = [i for i in range(1, amount) if counts[i] < largest] or [i for i in range(1, amount) if counts[i] < most]
        pool, left = sum([loads[i] for i in candidates]), spare
        for i in candidates:
            more = min(most - counts[i], max(1, left * loads[i] // pool), spare)
            counts[i] = counts[i] + more
            spare = spare - more
    return np.array(counts)


def noise(key, extent, scale, most, shards=(), held_as=jnp.bfloat16):
    array = jax.random.normal(key, extent, jnp.float32) * scale
    if len(shards) > 0:
        array = shard_levels(key, extent, shards, -0.22, 0.18) * array
    return jnp.clip(array, min=-most, max=most).astype(held_as)


def noise_with(key, dims, scale, limit, pieces, heavy, held_as=jnp.bfloat16):
    array = scale * jax.random.normal(key, dims, jnp.float32)
    if pieces:
        array = array * shard_levels(key, dims, pieces, -0.22, 0.18)
    return jnp.clip(raised(array, jax.random.fold_in(key, 3), *heavy), -limit, limit).astype(held_as)


def setup_inputs(seed: int = 0) -> dict:
    key_list = jax.random.split(jax.random.key(seed), 10)
    tokens = noise(key_list[0], (CLIENTS, TOK_CL, D), 1.0, 6.0, ((0, 8), (1, 32)))
    routes_keys = jax.random.split(jax.random.fold_in(key_list[1], 1), CLIENTS * TOK_CL // TOK_CL)
    routes_turns = jax.random.permutation(jax.random.fold_in(key_list[1], 3), CLIENTS * TOK_CL // TOK_CL)
    routes = jax.vmap(lambda own, number: routed_block(jax.random.fold_in(key_list[1], 2), own, number, TOK_CL, EXPERTS, 2, CAP, 1))(routes_keys, routes_turns).reshape((CLIENTS, TOK_CL, 2))
    router = noise(key_list[2], (D, EXPERTS), D ** -0.5, 0.09375)
    w_gate = noise(key_list[3], (EXPERTS, D, FF), D ** -0.5, 0.09375, ((0, 8), (2, 32)))
    w_up = noise(key_list[4], (EXPERTS, D, FF), D ** -0.5, 0.09375, ((0, 8), (2, 32)))
    w_down = noise_with(key_list[5], (EXPERTS, FF, D), FF ** -0.5, 0.109375, ((0, 8), (1, 32)), (1, 2, 32, 2.75))
    adapter = noise(key_list[6], (CLIENTS, D, D), D ** -0.5, 0.09375, ((0, 8), (2, 32)))
    upstream = draw_upstream(jax.random.fold_in(key_list[9], 71), 0)
    bound = jnp.clip(jnp.exp(math.log(16384.0) - 2.0794415 * jax.random.uniform(key_list[8], (CLIENTS,), jnp.float32) ** shard_levels(key_list[8], (CLIENTS,), ((0, 8),), -0.2, 0.2)), 2048.0, 16384.0)
    return {"tokens": tokens, "routes": routes, "router": router, "w_gate": w_gate, "w_up": w_up, "w_down": w_down, "adapter": adapter, "upstream": upstream, "bound": bound}


def slot_table(routed, expert_count):
    named_hits = lax.optimization_barrier(jnp.sum((routed[:, :, None] == jnp.arange(expert_count, dtype=jnp.int32)[None, None, :]).astype(jnp.int32), axis=1))
    before = jnp.cumsum(named_hits, axis=0) - named_hits
    return jnp.take_along_axis(before, routed, axis=1).astype(jnp.int32)

def pack_rows(token_rows, routed, expert_count, capacity):
    token_count = token_rows.shape[0]
    slot_flat = (routed * capacity + slot_table(routed, expert_count)).astype(jnp.int32)
    owners = jnp.repeat(jnp.arange(token_count, dtype=jnp.int32), 2)
    source = jnp.full((expert_count * capacity,), token_count, jnp.int32).at[slot_flat.reshape(-1)].set(owners)
    padded = jnp.concatenate([token_rows, jnp.zeros((1, token_rows.shape[1]), token_rows.dtype)], axis=0)
    return (padded[source].reshape(expert_count, capacity, token_rows.shape[1]), slot_flat)

def mix_weights(token_rows, routed, router):
    logits = jnp.dot(token_rows, router, preferred_element_type=jnp.float32)
    picked = jnp.take_along_axis(logits, routed, axis=1)
    weight_first = jax.nn.sigmoid(picked[:, 0] - picked[:, 1])
    return (weight_first, 1.0 - weight_first)

def reference(tokens, routes, router, w_gate, w_up, w_down, adapter, upstream, bound):

    def pack_one(token_rows, routed):
        return pack_rows(token_rows, routed, EXPERTS, CAP)
    packed, slot_flats = jax.vmap(pack_one)(tokens, routes)

    def add_block(running, operand_pair):
        down_piece = jnp.dot(operand_pair[0], operand_pair[1], preferred_element_type=jnp.float32).astype(jnp.bfloat16)
        down_piece = lax.optimization_barrier(down_piece)
        return (running + down_piece.astype(jnp.float32), None)

    def expert_one(inputs):
        expert_rows, gate_w, up_w, down_w = inputs
        flat_rows = expert_rows.reshape(-1, D)
        gate_out = jnp.dot(flat_rows, gate_w, preferred_element_type=jnp.float32)
        up_out = jnp.dot(flat_rows, up_w, preferred_element_type=jnp.float32)
        hidden = (jax.nn.silu(gate_out) * up_out).astype(jnp.bfloat16)
        blocks = jnp.transpose(hidden.reshape(-1, N_FFN, FF_DEV), (1, 0, 2))
        down_blocks = down_w.reshape(N_FFN, FF_DEV, D)
        running, _ = lax.scan(add_block, jnp.zeros((CLIENTS * CAP, D), jnp.float32), (blocks, down_blocks))
        return running.reshape(CLIENTS, CAP, D)
    expert_out = lax.map(expert_one, (jnp.moveaxis(packed, 1, 0), w_gate, w_up, w_down))
    by_client = jnp.moveaxis(expert_out, 0, 1).reshape(CLIENTS, EXPERTS * CAP, D)

    def client_one(inputs):
        token_rows, routed, slot_flat, expert_rows, adapt_matrix, grad_input, clip_limit = inputs
        weight_first, weight_second = mix_weights(token_rows, routed, router)
        picked = expert_rows[slot_flat]
        mixture = weight_first[:, None] * picked[:, 0] + weight_second[:, None] * picked[:, 1]
        layer_out = (token_rows.astype(jnp.float32) + mixture).astype(jnp.bfloat16)
        adapted = (layer_out.astype(jnp.float32) + jnp.dot(layer_out, adapt_matrix, preferred_element_type=jnp.float32)).astype(jnp.bfloat16)
        adapter_grad = lax.dot_general(layer_out, grad_input, (((0,), (0,)), ((), ())), preferred_element_type=jnp.float32)
        grad_norm = jnp.sqrt(jnp.sum(adapter_grad * adapter_grad))
        factor = clip_limit / jnp.maximum(grad_norm, clip_limit)
        return (adapted, (adapter_grad * factor).astype(jnp.bfloat16))
    adapted, clipped = lax.map(client_one, (tokens, routes, slot_flats, by_client, adapter, upstream, bound))
    return (adapted, clipped)
```

```python
import jax
import jax.numpy as jnp
from jax import lax
from jax.experimental import pallas as pl
from jax.experimental.pallas import tpu as pltpu
from jax.sharding import PartitionSpec as P

MESH = pl.DeviceIdType.MESH
BF = jnp.bfloat16
F32 = jnp.float32
NZ, NY = 8, 4
NF = NZ * NY
NE = 8
CAP = 48
TOK = 128
TF = TOK // NF
D = 4096
FD = 384
COL = 128
SLOTS = NE * CAP
R1 = 224
R2 = SLOTS - R1
Q1 = 80


def dot(a, b, dims=(((1,), (0,)), ((), ()))):
    return lax.dot_general(a, b, dims, preferred_element_type=F32)


def block(index):
    return pl.ds(pl.multiple_of(index * COL, COL), COL)


def add(*parts):
    total = parts[0].astype(F32)
    for part in parts[1:]:
        total = total + part.astype(F32)
    return total.astype(BF)


def kernel(
    tok_h, routes_h, router_h, gate_h, up_h, down_h, adapt_h, upstr_h, bound_ref,
    adapted_h, clipped_h,
    tok, routes, router, wg, wu, wd, adapt, upstr,
    xr, lr, ls, xf, lf, xc, a, ga, ua, pb, yb, ys, zb, z2, zs, w2, fin, rc, lay, grad, ns, nr, oa, oc,
    lsem, osem, a2a_s, a2a_r, log_s, log_r, pk_s, pk_r, rt_s, rt_r, nm_s, nm_r,
    ag_s, ag_r, rs_s, y_r, z_r, z2_r, w2_r, lg_s, lg_r,
):
    e = lax.axis_index("expert")
    f = lax.axis_index("ffn")
    z, y = f // NY, f % NY
    core = e % 2
    dm = 1 - 2 * core

    def zz(v):
        return (v + 2 * NZ) % NZ

    def yy(v):
        return (v + 2 * NY) % NY

    def at(zi, yi):
        return zi * NY + yi

    def sign(v):
        return 1 - 2 * ((v + core) % 2)

    def remote(src, dst, ss, rs, **where):
        return pltpu.make_async_remote_copy(
            src_ref=src, dst_ref=dst, send_sem=ss, recv_sem=rs,
            device_id=where, device_id_type=MESH,
        )

    loads = [
        pltpu.make_async_copy(src, dst, lsem.at[n])
        for n, (src, dst) in enumerate(
            ((tok_h, tok), (routes_h, routes), (router_h, router), (gate_h, wg), (up_h, wu),
             (down_h, wd), (upstr_h, upstr), (adapt_h, adapt))
        )
    ]
    for load in loads:
        load.start()

    barrier = pltpu.get_barrier_semaphore()

    @pl.loop(1, NF)
    def _(j):
        pl.semaphore_signal(barrier, inc=1, device_id={"ffn": (f + j) % NF}, device_id_type=MESH)

    @pl.loop(1, NE)
    def _(j):
        pl.semaphore_signal(barrier, inc=1, device_id={"expert": (e + j) % NE}, device_id_type=MESH)

    loads[0].wait()
    pl.semaphore_wait(barrier, NF - 1 + NE - 1)

    @pl.loop(1, NF)
    def _(j):
        peer = (f + j) % NF
        remote(tok.at[:, block(peer)], xr.at[f], a2a_s, a2a_r, ffn=peer).start()

    xr[f] = tok[:, block(f)]
    loads[2].wait()
    ls[...] = jnp.zeros_like(ls)
    ls[:, 0:NE] = dot(tok[...], router[...], (((1,), (1,)), ((), ())))

    @pl.loop(1, NF)
    def _(j):
        remote(ls, lr.at[f], log_s, log_r, ffn=(f + j) % NF).start()

    lr[f] = ls[...]

    loads[1].wait()
    r0, r1 = routes[0:1, :], routes[1:2, :]
    names = lax.broadcasted_iota(jnp.int32, (NE, TOK), 0)
    h0 = (names == r0).astype(F32)
    h1 = (names == r1).astype(F32)
    early = lax.broadcasted_iota(jnp.int32, (TOK, TOK), 0) < lax.broadcasted_iota(jnp.int32, (TOK, TOK), 1)
    before = dot((h0 + h1).astype(BF), early.astype(F32).astype(BF))
    slot0 = jnp.sum(before * h0, axis=0, keepdims=True).astype(jnp.int32) + r0 * CAP
    slot1 = jnp.sum(before * h1, axis=0, keepdims=True).astype(jnp.int32) + r1 * CAP
    places = lax.broadcasted_iota(jnp.int32, (SLOTS, TOK), 0)
    o0 = (places == slot0).astype(F32)
    o1 = (places == slot1).astype(F32)
    pick = (o0 + o1).astype(BF)

    others = pl.ds(0, NF - 1)
    remote(xr.at[others], xr.at[others], a2a_s, a2a_r, ffn=(f + 1) % NF).wait_recv()
    for n in range(NF):
        xf[TF * n:TF * (n + 1), :] = xr[n].astype(F32)
    xc[...] = dot(pick, xf[...].astype(BF)).astype(BF)

    mine = pl.ds(pl.multiple_of(e * CAP, CAP), CAP)

    @pl.loop(1, NE)
    def _(j):
        peer = (e + j) % NE
        theirs = pl.ds(pl.multiple_of(peer * CAP, CAP), CAP)
        remote(xc.at[theirs], a.at[mine, block(f)], pk_s, pk_r, expert=peer).start()

    a[mine, block(f)] = xc[mine, :]
    seven = pl.ds(0, CAP * (NE - 1))
    remote(xc.at[seven], rc.at[seven], pk_s, pk_r, expert=(e + 1) % NE).wait_recv()

    def gathered(buf, cut, total, ssem, rsem, on_chunk):
        sent = []
        rows = (pl.ds(0, cut), pl.ds(cut, total - cut))

        def piece(h, zi, yi, target):
            ref = buf.at[rows[h], block(at(zi, yi))]
            return remote(ref, ref, ssem.at[min(len(sent), 61)], rsem.at[h, at(zi, yi)], ffn=target)

        def send(h, zi, yi, zt, yt):
            copy = piece(h, zi, yi, at(zt, yt))
            copy.start()
            sent.append(copy)

        def wait(h, zi, yi):
            piece(h, zi, yi, at(zz(z + 1), y)).wait_recv()

        def to_y(h, zi, yi):
            send(h, zi, yi, z, yy(y + 1))
            send(h, zi, yi, z, yy(y - 1))

        def to_z(h, zi, yi):
            send(h, zi, yi, zz(z + 1), y)
            send(h, zi, yi, zz(z - 1), y)

        def first_z(k):
            def run():
                if k < 4:
                    for s in (1, -1):
                        wait(0, zz(z - s * k), y)
                        if k < 3:
                            send(0, zz(z - s * k), y, zz(z + s), y)
                    if k == 3:
                        send(0, zz(z - 3 * dm), y, zz(z + dm), y)
                    for s in (1, -1):
                        to_y(0, zz(z - s * k), y)
                else:
                    wait(0, zz(z + 4), y)
                    to_y(0, zz(z + 4), y)
            return run

        def then_y(off):
            def run():
                zi = zz(z + off)
                wait(0, zi, yy(y + 1))
                wait(0, zi, yy(y - 1))
                s = sign(zi)
                send(0, zi, yy(y - s), z, yy(y + s))
            return run

        def last_y(off):
            return lambda: wait(0, zz(z + off), yy(y + 2))

        def first_y(b):
            def run():
                wait(1, z, yy(y + b))
                to_z(1, z, yy(y + b))
            return run

        def then_z(b, k):
            def run():
                yi = yy(y + b)
                if k == 4:
                    wait(1, zz(z + 4), yi)
                    return
                for s in (1, -1):
                    wait(1, zz(z - s * k), yi)
                    if k < 3:
                        send(1, zz(z - s * k), yi, zz(z + s), y)
                if k == 3:
                    s = sign(yi)
                    send(1, zz(z - 3 * s), yi, zz(z + s), y)
            return run

        send(1, z, y, z, yy(y + 1))
        send(1, z, y, z, yy(y - 1))
        send(0, z, y, zz(z + 1), y)
        send(0, z, y, zz(z - 1), y)
        send(1, z, y, z, yy(y + 2))
        to_y(0, z, y)
        to_z(1, z, y)
        steps = [[] for _ in range(7)]
        for k in range(1, 5):
            steps[k].append(first_z(k))
        for b, r in ((1, 1), (-1, 1), (2, 2)):
            steps[r].append(first_y(b))
        for b, r in ((0, 0), (1, 1), (-1, 1), (2, 2)):
            for k in range(1, 5):
                steps[r + k].append(then_z(b, k))
        for off in (0, 1, -1, 2, -2, 3, -3, 4):
            steps[abs(off) + 1].append(then_y(off))
            steps[abs(off) + 2].append(last_y(off))
        for r in range(1, 7):
            for step in steps[r]:
                step()
            if r >= 2:
                for off in ((0,), (1, -1), (2, -2), (3, -3), (4,))[r - 2]:
                    on_chunk(zz(z + off), r == 2)
        for copy in sent:
            copy.wait_send()

    for n in (3, 4):
        loads[n].wait()

    def expert_chunk(zi, first):
        cols = pl.ds(pl.multiple_of(zi * NY * COL, NY * COL), NY * COL)
        x = a[:, cols]
        g, u = dot(x, wg[cols, :]), dot(x, wu[cols, :])
        if first:
            ga[...] = g
            ua[...] = u
        else:
            ga[...] += g
            ua[...] += u

    gathered(a, R1, SLOTS, ag_s, ag_r, expert_chunk)

    loads[5].wait()
    gate = ga[...]
    hidden = (gate / (1.0 + jnp.exp(-gate)) * ua[...]).astype(BF)

    @pl.loop(0, 8)
    def _(n):
        cols = pl.ds(pl.multiple_of(n * 512, 512), 512)
        pb[:, cols] = dot(hidden, wd[:, cols]).astype(BF)

    sent = []
    top, low = pl.ds(0, R1), pl.ds(R1, R2)

    def own(h, zi, yi):
        return pb.at[(top, low)[h], block(at(zi, yi))]

    def push(src, dst, rsem, zt, yt):
        copy = remote(src, dst, rs_s.at[len(sent)], rsem, ffn=at(zt, yt))
        copy.start()
        sent.append(copy)

    def got(dst, rsem):
        remote(dst, dst, rs_s.at[0], rsem, ffn=at(zz(z + 1), y)).wait_recv()

    offs = (4, 3 * dm, -3 * dm, 2 * dm, -2 * dm, dm, -dm, 0)

    def y1(i):
        zi = zz(z + offs[i])
        s = sign(zi)
        push(own(0, zi, yy(y + 2)), yb.at[i, 0], y_r.at[i, 0], z, yy(y + s))
        push(own(0, zi, yy(y - s)), yb.at[i, 2], y_r.at[i, 2], z, yy(y - s))

    def y2(i):
        zi = zz(z + offs[i])
        s = sign(zi)
        got(yb.at[i, 0], y_r.at[i, 0])
        yb[i, 0] = add(yb[i, 0], own(0, zi, yy(y + s))[...])
        push(yb.at[i, 0], yb.at[i, 1], y_r.at[i, 1], z, yy(y + s))

    def y3(i):
        zi = zz(z + offs[i])
        got(yb.at[i, 2], y_r.at[i, 2])
        got(yb.at[i, 1], y_r.at[i, 1])
        ys[i] = add(yb[i, 1], yb[i, 2], own(0, zi, y)[...])

    def z_first(i, slot, s):
        push(ys.at[i], zb.at[slot], z_r.at[slot], zz(z + s), y)

    def z_step(slot, i, to, s):
        got(zb.at[slot], z_r.at[slot])
        zb[slot] = add(zb[slot], ys[i])
        push(zb.at[slot], zb.at[to], z_r.at[to], zz(z + s), y)

    def z_last():
        got(zb.at[0], z_r.at[0])
        got(zb.at[4], z_r.at[4])
        fin[0:R1, :] = add(zb[0], zb[4], ys[7])

    boffs = (2, 1, -1, 0)

    def u1(j):
        yi = yy(y + boffs[j])
        s = sign(yi)
        push(own(1, zz(z + 4), yi), z2.at[j, 3], z2_r.at[j, 3], zz(z + s), y)
        push(own(1, zz(z - 3 * s), yi), z2.at[j, 6], z2_r.at[j, 6], zz(z - s), y)

    def u_step(j, r):
        yi = yy(y + boffs[j])
        s = sign(yi)
        k = 5 - r
        got(z2.at[j, k], z2_r.at[j, k])
        z2[j, k] = add(z2[j, k], own(1, zz(z + k * s), yi)[...])
        push(z2.at[j, k], z2.at[j, k - 1], z2_r.at[j, k - 1], zz(z + s), y)
        if k > 1:
            m = k - 1
            got(z2.at[j, 4 + m], z2_r.at[j, 4 + m])
            z2[j, 4 + m] = add(z2[j, 4 + m], own(1, zz(z - m * s), yi)[...])
            push(z2.at[j, 4 + m], z2.at[j, 3 + m], z2_r.at[j, 3 + m], zz(z - s), y)

    def u_last(j):
        yi = yy(y + boffs[j])
        got(z2.at[j, 0], z2_r.at[j, 0])
        got(z2.at[j, 4], z2_r.at[j, 4])
        zs[j] = add(z2[j, 0], z2[j, 4], own(1, z, yi)[...])
        if j < 3:
            push(zs.at[j], w2.at[j], w2_r.at[j], z, yi)

    def u_end():
        for j in range(3):
            got(w2.at[j], w2_r.at[j])
        fin[R1:SLOTS, :] = add(w2[0], w2[1], w2[2], zs[3])

    plan = []
    for i in range(8):
        plan.append((1.7 * (i - 1), lambda i=i: y1(i)))
        plan.append((1.84 * i + 3.2, lambda i=i: y2(i)))
        plan.append((1.84 * i + 6.2, lambda i=i: y3(i)))
    for when, run in (
        (6.5, lambda: z_first(0, 3, dm)),
        (9.9, lambda: z_first(2, 6, -dm)),
        (9.2, lambda: z_step(3, 1, 2, dm)),
        (12.2, lambda: z_step(2, 3, 1, dm)),
        (15.7, lambda: z_step(1, 5, 0, dm)),
        (13.9, lambda: z_step(6, 4, 5, -dm)),
        (17.5, lambda: z_step(5, 6, 4, -dm)),
        (20.0, z_last),
    ):
        plan.append((when, run))
    for j in range(4):
        plan.append((0.1 * j - 1.0, lambda j=j: u1(j)))
        for r in (2, 3, 4):
            plan.append((2.5 + 0.9 * j + 3.5 * (r - 2), lambda j=j, r=r: u_step(j, r)))
        plan.append((13.0 + 0.9 * j, lambda j=j: u_last(j)))
    plan.append((19.0, u_end))
    for _, run in sorted(plan, key=lambda item: item[0]):
        run()

    @pl.loop(1, NE)
    def _(j):
        peer = (e + j) % NE
        theirs = pl.ds(pl.multiple_of(peer * CAP, CAP), CAP)
        remote(fin.at[theirs], rc.at[mine], rt_s, rt_r, expert=peer).start()

    rc[mine, :] = fin[mine, :]
    remote(lr.at[others], lr.at[others], log_s, log_r, ffn=(f + 1) % NF).wait_recv()
    for n in range(NF):
        lf[TF * n:TF * (n + 1), :] = lr[n]
    logits = jnp.transpose(lf[...])[0:NE, :]
    gap = jnp.sum(logits * h0, axis=0, keepdims=True) - jnp.sum(logits * h1, axis=0, keepdims=True)
    weight0 = 1.0 / (1.0 + jnp.exp(-gap))
    share = o0 * weight0 + o1 * (1.0 - weight0)
    share_hi = share.astype(BF)
    share_lo = (share - share_hi.astype(F32)).astype(BF)
    first_dims = (((0,), (0,)), ((), ()))
    remote(fin.at[seven], rc.at[seven], rt_s, rt_r, expert=(e + 1) % NE).wait_recv()
    back = rc[...]
    mixture = dot(share_hi, back, first_dims) + dot(share_lo, back, first_dims)
    lay[:, block(f)] = (xf[...] + mixture).astype(BF)

    for n in (6, 7):
        loads[n].wait()
    oa_cols = []

    def adapter_chunk(zi, first):
        cols = pl.ds(pl.multiple_of(zi * NY * COL, NY * COL), NY * COL)
        x = lay[:, cols]
        g = dot(x, upstr[...], first_dims)
        grad[cols, :] = g
        part = jnp.sum((g * g).reshape(NY * COL // 8, 8, COL), axis=0)
        term = dot(x, adapt[cols, :])
        if first:
            ns[...] = part
            ga[0:TOK, 0:COL] = term
        else:
            ns[...] += part
            ga[0:TOK, 0:COL] += term

    gathered(lay, Q1, TOK, lg_s, lg_r, adapter_chunk)

    @pl.loop(1, NF)
    def _(j):
        remote(ns, nr.at[f], nm_s, nm_r, ffn=(f + j) % NF).start()

    nr[f] = ns[...]
    oa[...] = (lay[:, block(f)].astype(F32) + ga[0:TOK, 0:COL]).astype(BF)
    first_out = pltpu.make_async_copy(oa, adapted_h, osem.at[0])
    first_out.start()
    for copy in sent:
        copy.wait_send()
    remote(xr.at[others], xr.at[others], a2a_s, a2a_r, ffn=(f + 1) % NF).wait_send()
    remote(lr.at[others], lr.at[others], log_s, log_r, ffn=(f + 1) % NF).wait_send()
    remote(xc.at[seven], rc.at[seven], pk_s, pk_r, expert=(e + 1) % NE).wait_send()
    remote(fin.at[seven], rc.at[seven], rt_s, rt_r, expert=(e + 1) % NE).wait_send()
    norms = remote(nr.at[others], nr.at[others], nm_s, nm_r, ffn=(f + 1) % NF)
    norms.wait_recv()
    squared = jnp.sum(jnp.sum(nr[...], axis=0), keepdims=True)
    limit = bound_ref[0]
    factor = limit / jnp.maximum(jnp.sqrt(squared), limit)
    outs = []
    for n in range(4):
        part = slice(n * 1024, (n + 1) * 1024)
        oc[part, :] = (grad[part, :] * factor).astype(BF)
        out = pltpu.make_async_copy(oc.at[part, :], clipped_h.at[part, :], osem.at[1 + n])
        out.start()
        outs.append(out)
    norms.wait_send()
    first_out.wait()
    for out in outs:
        out.wait()


def per_device(tokens, routes, router, w_gate, w_up, w_down, adapter, upstream, bound):
    anywhere = pl.BlockSpec(memory_space=pl.ANY)
    vmem = pltpu.VMEM
    dma = pltpu.SemaphoreType.DMA
    adapted, clipped = pl.pallas_call(
        kernel,
        out_shape=(
            jax.ShapeDtypeStruct((TOK, COL), BF),
            jax.ShapeDtypeStruct((D, COL), BF),
        ),
        in_specs=[anywhere] * 8 + [pl.BlockSpec(memory_space=pltpu.SMEM)],
        out_specs=(anywhere, anywhere),
        scratch_shapes=[
            vmem((TF, D), BF), vmem((2, TOK), jnp.int32), vmem((NE, D), BF),
            vmem((D, FD), BF), vmem((D, FD), BF), vmem((FD, D), BF),
            vmem((D, COL), BF), vmem((TOK, COL), BF),
            vmem((NF, TF, COL), BF), vmem((NF, TF, COL), F32), vmem((TF, COL), F32),
            vmem((TOK, COL), F32), vmem((TOK, COL), F32),
            vmem((SLOTS, COL), BF), vmem((SLOTS, D), BF),
            vmem((SLOTS, FD), F32), vmem((SLOTS, FD), F32), vmem((SLOTS, D), BF),
            vmem((8, 3, R1, COL), BF), vmem((8, R1, COL), BF), vmem((7, R1, COL), BF),
            vmem((4, 7, R2, COL), BF), vmem((4, R2, COL), BF), vmem((3, R2, COL), BF),
            vmem((SLOTS, COL), BF), vmem((SLOTS, COL), BF),
            vmem((TOK, D), BF), vmem((D, COL), F32),
            vmem((8, COL), F32), vmem((NF, 8, COL), F32),
            vmem((TOK, COL), BF), vmem((D, COL), BF),
            dma((8,)), dma((5,)), dma, dma, dma, dma, dma, dma, dma, dma, dma, dma,
            dma((62,)), dma((2, NF)), dma((62,)), dma((8, 3)), dma((7,)), dma((4, 7)), dma((3,)),
            dma((62,)), dma((2, NF)),
        ],
        compiler_params=pltpu.CompilerParams(
            collective_id=0, has_side_effects=True, vmem_limit_bytes=60 * 1024 * 1024
        ),
    )(
        tokens[0], jnp.transpose(routes[0]), jnp.transpose(router), w_gate[0], w_up[0], w_down[0],
        adapter[0], upstream[0], bound,
    )
    return adapted[None], clipped[None]


def solution(mesh):
    placed = (
        P("expert", "ffn", None),
        P("expert", None, None),
        P(),
        P("expert", None, "ffn"),
        P("expert", None, "ffn"),
        P("expert", "ffn", None),
        P("expert", None, "ffn"),
        P("expert", None, "ffn"),
        P("expert"),
    )
    return jax.shard_map(
        per_device,
        mesh=mesh,
        in_specs=placed,
        out_specs=(P("expert", None, "ffn"), P("expert", None, "ffn")),
        check_vma=False,
    )
```

```python
import jax
import jax.numpy as jnp
from jax import lax
from jax.experimental import pallas as pl
from jax.experimental.pallas import tpu as pltpu
from jax.sharding import PartitionSpec as P

MESH = pl.DeviceIdType.MESH
BF = jnp.bfloat16
F32 = jnp.float32
NZ, NY = 8, 4
NF = NZ * NY
NE = 8
CAP = 48
TOK = 128
TF = TOK // NF
D = 4096
FD = 384
COL = 128
SLOTS = NE * CAP
GROUPS = (((0, 240, 1, True), (240, 144, 2, False)),)
WIDE = ((0, 80, 1, True), (80, 48, 2, True))
PARTS = tuple(part for group in GROUPS for part in group)
RATE = 46.6e3
FIRST_HOP, NEXT_HOP, LEAD = 2.2, 0.75, 0.8
BIAS, U_BIAS = (0.0, 0.0), 0.0


def dot(a, b, dims=(((1,), (0,)), ((), ()))):
    return lax.dot_general(a, b, dims, preferred_element_type=F32)


def block(index):
    return pl.ds(pl.multiple_of(index * COL, COL), COL)


def add(*parts):
    total = parts[0].astype(F32)
    for part in parts[1:]:
        total = total + part.astype(F32)
    return total.astype(BF)


def parity(v):
    return 1 if v % 2 == 0 else -1


def spread(kind, skip):
    out = []

    def along(b, s0):
        for s in (1, -1):
            out.append((0, b, s, 0))
            if skip:
                out.append((0, b, 2 * s, 0))
                out.append((-2 * s, b, s, 0))
                if s == s0:
                    out.append((-2 * s, b, 2 * s, 0))
            else:
                out.append((-s, b, s, 0))
                out.append((-2 * s, b, s, 0))
                if s == s0:
                    out.append((-3 * s, b, s, 0))

    if kind == 1:
        along(0, 1)
        for a in range(-3, 5):
            sg = parity(a)
            out.extend(((a, 0, 0, 1), (a, 0, 0, -1), (a, -sg, 0, sg)))
    else:
        out.extend(((0, 0, 0, 1), (0, 0, 0, -1), (0, 0, 0, 2)))
        for b in range(-1, 3):
            along(b, parity(b))
    return out


def wrap(a, b):
    return (a + 3) % 8 - 3, (b + 1) % 4 - 1


class Plan:
    def __init__(self):
        self.nodes = []
        self.waits = {}
        self.given = {}
        self.bias = 0.0

    def send(self, needs, makes, link, size, hops, act, wait, work=0.02):
        self.nodes.append(dict(needs=needs, makes=makes, link=link, cost=size / RATE, hops=hops, act=act, work=work, bias=self.bias))
        self.waits[makes] = wait

    def post(self, needs, makes, delay, act, wait, work=0.1):
        self.nodes.append(dict(needs=needs, makes=makes, link=None, delay=delay, act=act, work=work, bias=self.bias))
        self.waits[makes] = wait

    def compute(self, needs, makes, work, act):
        self.nodes.append(dict(needs=needs, makes=makes, link=None, delay=0.0, act=act, work=work, bias=self.bias))

    def order(self):
        users = {}
        for node in self.nodes:
            for need in node["needs"]:
                users.setdefault(need, []).append(node)
        length = {}

        def path(node):
            key = id(node)
            if key not in length:
                if node["link"] is None:
                    own = node["work"] + node["delay"]
                else:
                    own = node["work"] + node["cost"] * node["hops"] + FIRST_HOP + NEXT_HOP * (node["hops"] - 1)
                length[key] = own + max([path(user) for user in users.get(node["makes"], ())] or [0.0])
            return length[key]

        for node in self.nodes:
            path(node)
        known, free, core, busy, out = dict(self.given), {}, 0.0, (0.0, 0.0), []
        pending = list(self.nodes)
        while pending:
            best = None
            for at, node in enumerate(pending):
                if any(need not in known for need in node["needs"]):
                    continue
                ready = max([known[need] for need in node["needs"]] or [0.0])
                if node["link"] is None:
                    start = max(ready, core)
                else:
                    if busy[0] < ready < busy[1]:
                        ready = busy[1]
                    start = max(ready, free.get(node["link"], 0.0))
                key = (round(start, 2), node["link"] is None and node["work"] > 0.15, -length[id(node)] - node["bias"], at)
                if best is None or key < best[0]:
                    best = (key, node, ready, start)
            _, node, ready, start = best
            pending.remove(node)
            if node["link"] is None:
                core = start + node["work"]
                busy = (start, core)
                known[node["makes"]] = core + node["delay"]
                out.append((start, len(out), node))
            else:
                free[node["link"]] = start + node["cost"] * node["hops"]
                known[node["makes"]] = start + node["work"] + node["cost"] + FIRST_HOP + NEXT_HOP * (node["hops"] - 1)
                out.append((max(ready, start - LEAD), len(out), node))
        return [node for _, _, node in sorted(out, key=lambda item: item[:2])], max(known.values())

    def emit(self):
        order, _ = self.order()
        waited = set()
        for node in order:
            for need in node["needs"]:
                if need in self.waits and need not in waited:
                    waited.add(need)
                    self.waits[need]()
            node["act"]()
        for need, wait in self.waits.items():
            if need not in waited:
                wait()


def kernel(
    tok_h, routes_h, router_h, gate_h, up_h, down_h, adapt_h, upstr_h, bound_ref,
    adapted_h, clipped_h,
    tok, routes, router, wg, wu, wd, adapt, xr, lr, ls, xf, lf, xc, a, ga, ua, hid, pb, *rest,
):
    bufs, rest = rest[:len(PARTS)], rest[len(PARTS):]
    (fin, rc, lay, ups, acc, ones, ns, nr, factor, oa, oc,
     lsem, osem, a2a_s, a2a_r, log_s, log_r, pk_s, pk_r, rt_s, rt_r, nm_s, nm_r,
     ag_s, ag_r, rs_s, rs_r, lg_s, lg_r, ug_s, ug_r) = rest
    e = lax.axis_index("expert")
    f = lax.axis_index("ffn")
    z, y = f // NY, f % NY
    core = e % 2
    turn_z = {1: 1 - 2 * core, 2: 1 - 2 * ((y + core) % 2)}
    turn_y = {1: 1 - 2 * ((z + core) % 2), 2: 1}
    first_dims = (((0,), (0,)), ((), ()))

    def spot(kind, da, db):
        zi = (z + turn_z[kind] * da + 2 * NZ) % NZ
        yi = (y + turn_y[kind] * db + 2 * NY) % NY
        return zi * NY + yi

    def remote(src, dst, ss, rs, **where):
        return pltpu.make_async_remote_copy(
            src_ref=src, dst_ref=dst, send_sem=ss, recv_sem=rs,
            device_id=where, device_id_type=MESH,
        )

    def towards(da, db):
        return ("z", da > 0) if da else ("y", db > 0)

    loads = [
        pltpu.make_async_copy(src, dst, lsem.at[n])
        for n, (src, dst) in enumerate(
            ((tok_h, tok), (routes_h, routes), (router_h, router), (upstr_h, ups.at[:, block(f)]),
             (gate_h, wg), (up_h, wu), (down_h, wd), (adapt_h, adapt))
        )
    ]
    for load in loads:
        load.start()

    barrier = pltpu.get_barrier_semaphore()

    @pl.loop(1, NF)
    def _(j):
        pl.semaphore_signal(barrier, inc=1, device_id={"ffn": (f + j) % NF}, device_id_type=MESH)

    @pl.loop(1, NE)
    def _(j):
        pl.semaphore_signal(barrier, inc=1, device_id={"expert": (e + j) % NE}, device_id_type=MESH)

    loads[0].wait()
    pl.semaphore_wait(barrier, NF - 1 + NE - 1)

    plan = Plan()
    others = pl.ds(0, NF - 1)
    seven = pl.ds(0, CAP * (NE - 1))
    mine = pl.ds(pl.multiple_of(e * CAP, CAP), CAP)
    next_f, next_e = (f + 1) % NF, (e + 1) % NE

    def loaded(n):
        plan.waits["load", n] = loads[n].wait
        plan.given["load", n] = 0.0
        return "load", n

    def to_columns():
        @pl.loop(1, NF)
        def _(j):
            peer = (f + j) % NF
            remote(tok.at[:, block(peer)], xr.at[f], a2a_s, a2a_r, ffn=peer).start()

        xr[f] = tok[:, block(f)]

    columns = remote(xr.at[others], xr.at[others], a2a_s, a2a_r, ffn=next_f)
    plan.post([], "columns", 4.6, to_columns, columns.wait_recv, 0.2)

    def own_logits():
        loads[2].wait()
        ls[...] = jnp.zeros_like(ls)
        ls[:, 0:NE] = dot(tok[...], router[...], (((1,), (1,)), ((), ())))

        @pl.loop(1, NF)
        def _(j):
            remote(ls, lr.at[f], log_s, log_r, ffn=(f + j) % NF).start()

        lr[f] = ls[...]

    everyone = remote(lr.at[others], lr.at[others], log_s, log_r, ffn=next_f)
    plan.post([], "logits", 6.0, own_logits, everyone.wait_recv, 0.55)

    def own_slots():
        loads[1].wait()
        r0, r1 = routes[0:1, :], routes[1:2, :]
        names = lax.broadcasted_iota(jnp.int32, (NE, TOK), 0)
        h0 = (names == r0).astype(F32)
        h1 = (names == r1).astype(F32)
        early = lax.broadcasted_iota(jnp.int32, (TOK, TOK), 0) < lax.broadcasted_iota(jnp.int32, (TOK, TOK), 1)
        before = dot((h0 + h1).astype(BF), early.astype(F32).astype(BF))
        slot0 = jnp.sum(before * h0, axis=0, keepdims=True).astype(jnp.int32) + r0 * CAP
        slot1 = jnp.sum(before * h1, axis=0, keepdims=True).astype(jnp.int32) + r1 * CAP
        places = lax.broadcasted_iota(jnp.int32, (SLOTS, TOK), 0)
        ones[0] = (places == slot0).astype(F32)
        ones[1] = (places == slot1).astype(F32)

    plan.compute([], "slots", 0.2, own_slots)

    def pack():
        for n in range(NF):
            xf[TF * n:TF * (n + 1), :] = xr[n].astype(F32)
        xc[...] = dot((ones[0] + ones[1]).astype(BF), xf[...].astype(BF)).astype(BF)

        @pl.loop(1, NE)
        def _(j):
            peer = (e + j) % NE
            theirs = pl.ds(pl.multiple_of(peer * CAP, CAP), CAP)
            remote(xc.at[theirs], a.at[mine, block(f)], pk_s, pk_r, expert=peer).start()

        a[mine, block(f)] = xc[mine, :]

    packed = remote(xc.at[seven], rc.at[seven], pk_s, pk_r, expert=next_e)
    plan.post(["columns", "slots"], "packed", 4.3, pack, packed.wait_recv, 0.2)

    def gather(name, buf, parts, ssem, rsem, start, chunk_work, on_chunk, extra=(), before=()):
        pieces = {}
        for p, (row, rows, kind, skip) in enumerate(parts):
            for da, db, sa, sb in spread(kind, skip):
                def act(p=p, row=row, rows=rows, kind=kind, da=da, db=db, sa=sa, sb=sb):
                    ref = buf.at[pl.ds(row, rows), block(spot(kind, da, db))]
                    remote(ref, ref, ssem.at[p], rsem.at[p, spot(kind, da, db)], ffn=spot(kind, sa, sb)).start()

                ra, rb = wrap(da - sa, db - sb)

                def wait(p=p, row=row, rows=rows, kind=kind, ra=ra, rb=rb):
                    ref = buf.at[pl.ds(row, rows), block(spot(kind, ra, rb))]
                    remote(ref, ref, ssem.at[p], rsem.at[p, spot(kind, ra, rb)], ffn=next_f).wait_recv()

                held = (name, p, da, db) if (da, db) != (0, 0) else start
                makes = (name, p, ra, rb)
                pieces.setdefault(abs(ra), []).append(makes)
                plan.send([held, *before], makes, towards(sa, sb), rows * COL * 2, abs(sa) + abs(sb), act, wait)
        for k in range(5):
            for s in ((1,) if k in (0, 4) else (1, -1)):
                needs = [start, *pieces[k], *extra]
                if k:
                    needs.append((name, "chunk", 0, 1))
                plan.compute(needs, (name, "chunk", k, s), chunk_work,
                             lambda k=k, s=s: on_chunk((z + s * k + NZ) % NZ, k == 0))
        return [(name, "chunk", k, s) for k in range(5) for s in ((1,) if k in (0, 4) else (1, -1))]

    def gather_done(buf, parts, ssem):
        for p, (row, rows, _, _) in enumerate(parts):
            ref = buf.at[pl.ds(row, rows), pl.ds(0, COL * (NF - 1))]
            remote(ref, ref, ssem.at[p], lg_r.at[0, 0], ffn=next_f).wait_send()

    plan.bias = U_BIAS
    ups_all = gather("u", ups, WIDE, ug_s, ug_r, loaded(3), 0.0, lambda zi, first: None)

    fins = []
    for g, group in enumerate(GROUPS):
        base, size = group[0][0], sum(part[1] for part in group)
        span = pl.ds(base, size)
        plan.bias = BIAS[g]

        def expert_chunk(zi, first, span=span):
            cols = pl.ds(pl.multiple_of(zi * NY * COL, NY * COL), NY * COL)
            x = a[span, cols]
            left, right = dot(x, wg[cols, :]), dot(x, wu[cols, :])
            if first:
                ga[span, :] = left
                ua[span, :] = right
            else:
                ga[span, :] += left
                ua[span, :] += right

        sub = [ag_s.at[pl.ds(2 * g, 2)], ag_r.at[pl.ds(2 * g, 2)]]
        chunks = gather(("x", g), a, group, *sub, "packed", 0.45 * size / SLOTS + 0.05, expert_chunk,
                        (loaded(4), loaded(5)))

        def hide(span=span):
            gate = ga[span, :]
            hid[span, :] = (gate / (1.0 + jnp.exp(-gate)) * ua[span, :]).astype(BF)

        plan.compute(chunks, ("hid", g), 0.5 * size / SLOTS, hide)
        for k in (4, 3, 2, 1, 0):
            def down(k=k, span=span):
                for s in ((1,) if k in (0, 4) else (1, -1)):
                    zi = (z + s * k + NZ) % NZ
                    cols = pl.ds(pl.multiple_of(zi * NY * COL, NY * COL), NY * COL)
                    pb[span, cols] = dot(hid[span, :], wd[:, cols]).astype(BF)

            plan.compute([("hid", g), loaded(6)], ("pb", g, k), (0.3 if k in (0, 4) else 0.6) * size / SLOTS, down)

        for p, (row, rows, kind, skip) in enumerate(group):
            buf, q = bufs[2 * g + p], 2 * g + p
            slots = {}

            def slot(key, slots=slots):
                return slots.setdefault(key, len(slots))

            def own(da, db, row=row, rows=rows, kind=kind):
                return pb.at[pl.ds(row, rows), block(spot(kind, da, db))]

            def hop(key, needs, parts, sa, sb, buf=buf, q=q, kind=kind, rows=rows, slot=slot):
                to = slot(key)

                def act():
                    refs = [part() for part in parts]
                    if len(refs) > 1:
                        refs[0][...] = add(*[ref[...] for ref in refs])
                    remote(refs[0], buf.at[to], rs_s.at[q], rs_r.at[q, to], ffn=spot(kind, sa, sb)).start()

                def wait():
                    remote(buf.at[to], buf.at[to], rs_s.at[q], rs_r.at[q, to], ffn=next_f).wait_recv()

                plan.send(needs, (q, key), towards(sa, sb), rows * COL * 2, abs(sa) + abs(sb), act, wait,
                          0.02 if len(parts) == 1 else 0.08)

            def here(key, buf=buf, slot=slot):
                return lambda: buf.at[slot(key)]

            def total(makes, needs, parts, out, q=q):
                def act():
                    out()[...] = add(*[part()[...] for part in parts])

                plan.compute(needs, makes, 0.1, act)

            def mid(n, buf=buf):
                return lambda: buf.at[31 + n]

            def mine_at(da, db, own=own):
                return lambda: own(da, db)

            done = ("fin", q)
            final = lambda row=row, rows=rows: fin.at[pl.ds(row, rows), :]
            if kind == 1:
                for da in range(-3, 5):
                    sg, ready = parity(da), ("pb", g, abs(da))
                    hop(("y0", da), [ready], [mine_at(da, 2)], 0, sg)
                    hop(("y2", da), [ready], [mine_at(da, -sg)], 0, -sg)
                    hop(("y1", da), [ready, (q, ("y0", da))], [here(("y0", da)), mine_at(da, sg)], 0, sg)
                    total((q, "sum", da), [ready, (q, ("y1", da)), (q, ("y2", da))],
                          [here(("y1", da)), here(("y2", da)), mine_at(da, 0)], mid(da + 3))
                for s in (1, -1):
                    far = [(q, ("z3", s))] + ([(q, ("z4", s))] if s == 1 else [])
                    if s == 1:
                        hop(("z4", s), [(q, "sum", 4)], [mid(7)], 2, 0)
                    hop(("z3", s), [(q, "sum", 3 * s)], [mid(3 * s + 3)], s, 0)
                    hop(("z2", s), [(q, "sum", 2 * s), *far],
                        [here(("z3", s)), mid(2 * s + 3)] + ([here(("z4", s))] if s == 1 else []), 2 * s, 0)
                    hop(("z1", s), [(q, "sum", s)], [mid(s + 3)], s, 0)
                ends = [("z2", 1), ("z2", -1), ("z1", 1), ("z1", -1)]
                total(done, [(q, "sum", 0)] + [(q, end) for end in ends], [mid(3)] + [here(end) for end in ends], final)
            else:
                for db in range(-1, 3):
                    for s in (1, -1):
                        last = 4 if s == parity(db) else 3
                        for k in range(last, 0, -1):
                            ready = ("pb", g, k)
                            if k == last:
                                hop(("v", db, s, k - 1), [ready], [mine_at(s * k, db)], s, 0)
                            else:
                                hop(("v", db, s, k - 1), [ready, (q, ("v", db, s, k))],
                                    [here(("v", db, s, k)), mine_at(s * k, db)], s, 0)
                    total((q, "sum", db), [("pb", g, 0), (q, ("v", db, 1, 0)), (q, ("v", db, -1, 0))],
                          [mine_at(0, db), here(("v", db, 1, 0)), here(("v", db, -1, 0))], mid(db + 1))
                    if db:
                        hop(("w", db), [(q, "sum", db)], [mid(db + 1)], 0, db)
                total(done, [(q, "sum", 0)] + [(q, ("w", db)) for db in (1, -1, 2)],
                      [mid(1)] + [here(("w", db)) for db in (1, -1, 2)], final)
            fins.append(done)

    plan.bias = 0.0

    def give_back():
        @pl.loop(1, NE)
        def _(j):
            peer = (e + j) % NE
            theirs = pl.ds(pl.multiple_of(peer * CAP, CAP), CAP)
            remote(fin.at[theirs], rc.at[mine], rt_s, rt_r, expert=peer).start()

        rc[mine, :] = fin[mine, :]

    returned = remote(fin.at[seven], rc.at[seven], rt_s, rt_r, expert=next_e)
    plan.post(fins, "back", 4.3, give_back, returned.wait_recv, 0.1)

    def weigh():
        for n in range(NF):
            lf[TF * n:TF * (n + 1), :] = lr[n]
        logits = jnp.transpose(lf[...])[0:NE, :]
        names = lax.broadcasted_iota(jnp.int32, (NE, TOK), 0)
        gap = jnp.sum(logits * (names == routes[0:1, :]).astype(F32), axis=0, keepdims=True)
        gap = gap - jnp.sum(logits * (names == routes[1:2, :]).astype(F32), axis=0, keepdims=True)
        weight0 = 1.0 / (1.0 + jnp.exp(-gap))
        ones[0] = ones[0] * weight0 + ones[1] * (1.0 - weight0)

    plan.compute(["logits", "packed"], "share", 0.5, weigh)

    def combine():
        share = ones[0]
        share_hi = share.astype(BF)
        share_lo = (share - share_hi.astype(F32)).astype(BF)
        back = rc[...]
        mixture = dot(share_hi, back, first_dims) + dot(share_lo, back, first_dims)
        lay[:, block(f)] = (xf[...] + mixture).astype(BF)

    plan.compute(["back", "share"], "layer", 0.3, combine)

    def square():
        own_t = jnp.transpose(lay[:, block(f)].astype(F32)).astype(BF)
        total = jnp.zeros((TOK, COL), F32)
        for n in range(NZ):
            part = dot(own_t, ups[:, n * NY * COL:(n + 1) * NY * COL])
            part = part * part
            total = total + (part[:, 0:128] + part[:, 128:256]) + (part[:, 256:384] + part[:, 384:512])
        ns[...] = jnp.sum(total.reshape(16, 8, COL), axis=0)

        @pl.loop(1, NF)
        def _(j):
            remote(ns, nr.at[f], nm_s, nm_r, ffn=(f + j) % NF).start()

        nr[f] = ns[...]

    norms = remote(nr.at[others], nr.at[others], nm_s, nm_r, ffn=next_f)
    plan.post(["layer", ("early", 0), *ups_all], "norms", 6.0, square, norms.wait_recv, 0.6)

    def scale():
        squared = jnp.sum(jnp.sum(nr[...], axis=0), keepdims=True)
        limit = bound_ref[0]
        factor[...] = jnp.broadcast_to(limit / jnp.maximum(jnp.sqrt(squared), limit), (8, COL))

    plan.compute(["norms"], "factor", 0.2, scale)
    outs = []

    def adapter_chunk(zi, first):
        cols = pl.ds(pl.multiple_of(zi * NY * COL, NY * COL), NY * COL)
        x = lay[:, cols]
        grad = dot(x, ups[:, block(f)], first_dims)
        oc[cols, :] = (grad * factor[0:1, :]).astype(BF)
        out = pltpu.make_async_copy(oc.at[cols, :], clipped_h.at[cols, :], osem.at[1 + len(outs)])
        out.start()
        outs.append(out)
        term = dot(x, adapt[cols, :])
        if first:
            acc[...] = term
        else:
            acc[...] += term

    plan.compute(["layer"], ("early", 0), 0.01, lambda: None)
    gather("l", lay, WIDE, lg_s, lg_r, "layer", 0.16, adapter_chunk, ("factor", loaded(7)))
    plan.emit()

    oa[...] = (lay[:, block(f)].astype(F32) + acc[...]).astype(BF)
    first_out = pltpu.make_async_copy(oa, adapted_h, osem.at[0])
    first_out.start()
    columns.wait_send()
    everyone.wait_send()
    packed.wait_send()
    returned.wait_send()
    norms.wait_send()
    gather_done(ups, WIDE, ug_s)
    gather_done(lay, WIDE, lg_s)
    gather_done(a, PARTS, ag_s)
    for q, (_, rows, _, _) in enumerate(PARTS):
        ref = bufs[q].at[pl.ds(0, NF - 1)]
        remote(ref, ref, rs_s.at[q], rs_r.at[q, 0], ffn=next_f).wait_send()
    first_out.wait()
    for out in outs:
        out.wait()


def pass_on(adapted_h, clipped_h, adapted_out, clipped_out, held, small, sem_in, sem_out):
    steps = [(adapted_h, small, adapted_out)]
    for n in range(4):
        part = pl.ds(n * D // 4, D // 4)
        steps.append((clipped_h.at[part, :], held.at[part, :], clipped_out.at[part, :]))
    ins = [pltpu.make_async_copy(src, mid, sem_in.at[n]) for n, (src, mid, _) in enumerate(steps)]
    outs = [pltpu.make_async_copy(mid, dst, sem_out.at[n]) for n, (_, mid, dst) in enumerate(steps)]
    for copy in ins:
        copy.start()
    for copy, out in zip(ins, outs):
        copy.wait()
        out.start()
    for out in outs:
        out.wait()


def per_device(tokens, routes, router, w_gate, w_up, w_down, adapter, upstream, bound):
    anywhere = pl.BlockSpec(memory_space=pl.ANY)
    vmem = pltpu.VMEM
    dma = pltpu.SemaphoreType.DMA
    adapted, clipped = pl.pallas_call(
        kernel,
        out_shape=(
            jax.ShapeDtypeStruct((TOK, COL), BF),
            jax.ShapeDtypeStruct((D, COL), BF),
        ),
        in_specs=[anywhere] * 8 + [pl.BlockSpec(memory_space=pltpu.SMEM)],
        out_specs=(anywhere, anywhere),
        scratch_shapes=[
            vmem((TF, D), BF), vmem((2, TOK), jnp.int32), vmem((NE, D), BF),
            vmem((D, FD), BF), vmem((D, FD), BF), vmem((FD, D), BF), vmem((D, COL), BF),
            vmem((NF, TF, COL), BF), vmem((NF, TF, COL), F32), vmem((TF, COL), F32),
            vmem((TOK, COL), F32), vmem((TOK, COL), F32),
            vmem((SLOTS, COL), BF), vmem((SLOTS, D), BF),
            vmem((SLOTS, FD), F32), vmem((SLOTS, FD), F32), vmem((SLOTS, FD), BF), vmem((SLOTS, D), BF),
            *[vmem((39, part[1], COL), BF) for part in PARTS],
            vmem((SLOTS, COL), BF), vmem((SLOTS, COL), BF),
            vmem((TOK, D), BF), vmem((TOK, D), BF), vmem((TOK, COL), F32), vmem((2, SLOTS, TOK), F32),
            vmem((8, COL), F32), vmem((NF, 8, COL), F32), vmem((8, COL), F32),
            vmem((TOK, COL), BF), vmem((D, COL), BF),
            dma((8,)), dma((9,)), dma, dma, dma, dma, dma, dma, dma, dma, dma, dma,
            dma((len(PARTS),)), dma((len(PARTS), NF)), dma((len(PARTS),)), dma((len(PARTS), NF - 1)),
            dma((2,)), dma((2, NF)), dma((2,)), dma((2, NF)),
        ],
        compiler_params=pltpu.CompilerParams(
            collective_id=0, has_side_effects=True, vmem_limit_bytes=60 * 1024 * 1024
        ),
    )(
        tokens[0], jnp.transpose(routes[0]), jnp.transpose(router), w_gate[0], w_up[0], w_down[0],
        adapter[0], upstream[0], bound,
    )
    shapes = (jax.ShapeDtypeStruct((TOK, COL), BF), jax.ShapeDtypeStruct((D, COL), BF))
    adapted, clipped = pl.pallas_call(
        pass_on,
        out_shape=shapes,
        in_specs=[anywhere] * 2,
        out_specs=(anywhere, anywhere),
        scratch_shapes=[vmem((D, COL), BF), vmem((TOK, COL), BF), dma((5,)), dma((5,))],
    )(adapted, clipped)
    return adapted[None], clipped[None]


def solution(mesh):
    placed = (
        P("expert", "ffn", None),
        P("expert", None, None),
        P(),
        P("expert", None, "ffn"),
        P("expert", None, "ffn"),
        P("expert", "ffn", None),
        P("expert", None, "ffn"),
        P("expert", None, "ffn"),
        P("expert"),
    )
    return jax.shard_map(
        per_device,
        mesh=mesh,
        in_specs=placed,
        out_specs=(P("expert", None, "ffn"), P("expert", None, "ffn")),
        check_vma=False,
    )
```

```python
import jax
import jax.numpy as jnp
from jax import lax
from jax.experimental import pallas as pl
from jax.experimental.pallas import tpu as pltpu
from jax.sharding import PartitionSpec as P

MESH = pl.DeviceIdType.MESH
BF = jnp.bfloat16
F32 = jnp.float32
NZ, NY = 8, 4
NF = NZ * NY
NE = 8
CAP = 48
TOK = 128
TF = TOK // NF
D = 4096
FD = 384
COL = 128
SLOTS = NE * CAP
GROUPS = (((0, 240, 1, 1, 0), (240, 144, 2, 0, 1)),)
WIDE = ((0, 80, 1, 1, 0), (80, 48, 2, 1, 1))
LAST = ((0, 80, 1, 1, 1), (80, 48, 2, 1, 1))
PARTS = tuple(part for group in GROUPS for part in group)
RATE = {("z", True): 50e3, ("z", False): 43e3, ("y", True): 48.5e3, ("y", False): 44.5e3}
FIRST_HOP, NEXT_HOP, LEAD = 3.0, 0.75, 0.8
BIAS, U_BIAS = (0.0, 0.0), 0.0
U_AFTER = ()


def dot(a, b, dims=(((1,), (0,)), ((), ()))):
    return lax.dot_general(a, b, dims, preferred_element_type=F32)


def block(index):
    return pl.ds(pl.multiple_of(index * COL, COL), COL)


def add(*parts):
    total = parts[0].astype(F32)
    for part in parts[1:]:
        total = total + part.astype(F32)
    return total.astype(BF)


def parity(v):
    return 1 if v % 2 == 0 else -1


def spread(kind, zmode, ymode):
    out = []

    def along(b, s0):
        for s in (1, -1):
            out.append((0, b, s, 0))
            if zmode == 2:
                out.extend(((0, b, 2 * s, 0), (0, b, 3 * s, 0)))
                if s == s0:
                    out.append((0, b, 4 * s, 0))
            elif zmode == 1:
                out.extend(((0, b, 2 * s, 0), (-2 * s, b, s, 0)))
                if s == s0:
                    out.append((-2 * s, b, 2 * s, 0))
            else:
                out.extend(((-s, b, s, 0), (-2 * s, b, s, 0)))
                if s == s0:
                    out.append((-3 * s, b, s, 0))

    if kind == 1:
        along(0, 1)
        for a in range(-3, 5):
            sg = parity(a)
            out.extend(((a, 0, 0, 1), (a, 0, 0, -1), (a, 0, 0, 2 * sg) if ymode else (a, -sg, 0, sg)))
    else:
        out.extend(((0, 0, 0, 1), (0, 0, 0, -1), (0, 0, 0, 2)))
        for b in range(-1, 3):
            along(b, parity(b))
    return out


def wrap(a, b):
    return (a + 3) % 8 - 3, (b + 1) % 4 - 1


class Plan:
    def __init__(self):
        self.nodes = []
        self.waits = {}
        self.given = {}
        self.bias = 0.0

    def send(self, needs, makes, link, size, hops, act, wait, work=0.02):
        self.nodes.append(dict(needs=needs, makes=makes, link=link, cost=size / RATE[link], hops=hops, act=act, work=work, bias=self.bias))
        self.waits[makes] = wait

    def post(self, needs, makes, delay, act, wait, work=0.1):
        self.nodes.append(dict(needs=needs, makes=makes, link=None, delay=delay, act=act, work=work, bias=self.bias))
        self.waits[makes] = wait

    def compute(self, needs, makes, work, act):
        self.nodes.append(dict(needs=needs, makes=makes, link=None, delay=0.0, act=act, work=work, bias=self.bias))

    def order(self):
        users = {}
        for node in self.nodes:
            for need in node["needs"]:
                users.setdefault(need, []).append(node)
        length = {}

        def path(node):
            key = id(node)
            if key not in length:
                if node["link"] is None:
                    own = node["work"] + node["delay"]
                else:
                    own = node["work"] + node["cost"] * node["hops"] + FIRST_HOP + NEXT_HOP * (node["hops"] - 1)
                length[key] = own + max([path(user) for user in users.get(node["makes"], ())] or [0.0])
            return length[key]

        for node in self.nodes:
            path(node)
        known, free, core, busy, out = dict(self.given), {}, 0.0, (0.0, 0.0), []
        pending = list(self.nodes)
        while pending:
            best = None
            for at, node in enumerate(pending):
                if any(need not in known for need in node["needs"]):
                    continue
                ready = max([known[need] for need in node["needs"]] or [0.0])
                if node["link"] is None:
                    start = max(ready, core)
                else:
                    if busy[0] < ready < busy[1]:
                        ready = busy[1]
                    start = max(ready, free.get(node["link"], 0.0))
                key = (round(start, 2), node["link"] is None and node["work"] > 0.15, -length[id(node)] - node["bias"], at)
                if best is None or key < best[0]:
                    best = (key, node, ready, start)
            _, node, ready, start = best
            pending.remove(node)
            if node["link"] is None:
                core = start + node["work"]
                busy = (start, core)
                known[node["makes"]] = core + node["delay"]
                out.append((start, len(out), node))
            else:
                free[node["link"]] = start + node["cost"] * node["hops"]
                known[node["makes"]] = start + node["work"] + node["cost"] + FIRST_HOP + NEXT_HOP * (node["hops"] - 1)
                out.append((max(ready, start - LEAD), len(out), node))
        return [node for _, _, node in sorted(out, key=lambda item: item[:2])], max(known.values())

    def emit(self):
        order, _ = self.order()
        waited = set()
        for node in order:
            for need in node["needs"]:
                if need in self.waits and need not in waited:
                    waited.add(need)
                    self.waits[need]()
            node["act"]()
        for need, wait in self.waits.items():
            if need not in waited:
                wait()


def kernel(
    tok_h, routes_h, router_h, gate_h, up_h, down_h, adapt_h, upstr_h, bound_ref,
    adapted_h, clipped_h,
    tok, routes, router, wg, wu, wd, adapt, xr, lr, ls, xf, lf, xc, a, ga, ua, hid, pb, *rest,
):
    bufs, rest = rest[:len(PARTS)], rest[len(PARTS):]
    (fin, rc, lay, ups, acc, ones, ns, nr, factor, oa, oc,
     lsem, osem, a2a_s, a2a_r, log_s, log_r, pk_s, pk_r, rt_s, rt_r, nm_s, nm_r,
     ag_s, ag_r, rs_s, rs_r, lg_s, lg_r, ug_s, ug_r) = rest
    e = lax.axis_index("expert")
    f = lax.axis_index("ffn")
    z, y = f // NY, f % NY
    core = e % 2
    turn = 1 - 2 * core
    turn_y = {1: turn, 2: 1}
    first_dims = (((0,), (0,)), ((), ()))

    def spot(kind, da, db):
        zi = (z + turn * da + 2 * NZ) % NZ
        yi = (y + turn_y[kind] * db + 2 * NY) % NY
        return zi * NY + yi

    def remote(src, dst, ss, rs, **where):
        return pltpu.make_async_remote_copy(
            src_ref=src, dst_ref=dst, send_sem=ss, recv_sem=rs,
            device_id=where, device_id_type=MESH,
        )

    def towards(da, db):
        return ("z", da > 0) if da else ("y", db > 0)

    loads = [
        pltpu.make_async_copy(src, dst, lsem.at[n])
        for n, (src, dst) in enumerate(
            ((tok_h, tok), (routes_h, routes), (router_h, router), (upstr_h, ups.at[:, block(f)]),
             (gate_h, wg), (up_h, wu), (down_h, wd), (adapt_h, adapt))
        )
    ]
    for load in loads:
        load.start()

    barrier = pltpu.get_barrier_semaphore()

    @pl.loop(1, NF)
    def _(j):
        pl.semaphore_signal(barrier, inc=1, device_id={"ffn": (f + j) % NF}, device_id_type=MESH)

    @pl.loop(1, NE)
    def _(j):
        pl.semaphore_signal(barrier, inc=1, device_id={"expert": (e + j) % NE}, device_id_type=MESH)

    loads[0].wait()
    pl.semaphore_wait(barrier, NF - 1 + NE - 1)

    plan = Plan()
    others = pl.ds(0, NF - 1)
    seven = pl.ds(0, CAP * (NE - 1))
    mine = pl.ds(pl.multiple_of(e * CAP, CAP), CAP)
    next_f, next_e = (f + 1) % NF, (e + 1) % NE

    peers = [(e // 2 + chip) % (NE // 2) * 2 + other for chip in (2, 1, 3) for other in (0, 1)] + [e + turn]

    def theirs(peer):
        return pl.ds(pl.multiple_of(peer * CAP, CAP), CAP)

    def loaded(n):
        plan.waits["load", n] = loads[n].wait
        plan.given["load", n] = 0.0
        return "load", n

    def to_columns():
        @pl.loop(1, NF)
        def _(j):
            peer = (f + j) % NF
            remote(tok.at[:, block(peer)], xr.at[f], a2a_s, a2a_r, ffn=peer).start()

        xr[f] = tok[:, block(f)]

    columns = remote(xr.at[others], xr.at[others], a2a_s, a2a_r, ffn=next_f)
    plan.post([], "columns", 4.6, to_columns, columns.wait_recv, 0.2)

    def own_logits():
        loads[2].wait()
        ls[...] = jnp.zeros_like(ls)
        ls[:, 0:NE] = dot(tok[...], router[...], (((1,), (1,)), ((), ())))

        @pl.loop(1, NF)
        def _(j):
            remote(ls, lr.at[f], log_s, log_r, ffn=(f + j) % NF).start()

        lr[f] = ls[...]

    everyone = remote(lr.at[others], lr.at[others], log_s, log_r, ffn=next_f)
    plan.post([], "logits", 6.0, own_logits, everyone.wait_recv, 0.55)

    def own_slots():
        loads[1].wait()
        r0, r1 = routes[0:1, :], routes[1:2, :]
        names = lax.broadcasted_iota(jnp.int32, (NE, TOK), 0)
        h0 = (names == r0).astype(F32)
        h1 = (names == r1).astype(F32)
        early = lax.broadcasted_iota(jnp.int32, (TOK, TOK), 0) < lax.broadcasted_iota(jnp.int32, (TOK, TOK), 1)
        before = dot((h0 + h1).astype(BF), early.astype(F32).astype(BF))
        slot0 = jnp.sum(before * h0, axis=0, keepdims=True).astype(jnp.int32) + r0 * CAP
        slot1 = jnp.sum(before * h1, axis=0, keepdims=True).astype(jnp.int32) + r1 * CAP
        places = lax.broadcasted_iota(jnp.int32, (SLOTS, TOK), 0)
        ones[0] = (places == slot0).astype(F32)
        ones[1] = (places == slot1).astype(F32)

    plan.compute([], "slots", 0.2, own_slots)

    def pack():
        for n in range(NF):
            xf[TF * n:TF * (n + 1), :] = xr[n].astype(F32)
        xc[...] = dot((ones[0] + ones[1]).astype(BF), xf[...].astype(BF)).astype(BF)

        for peer in peers:
            remote(xc.at[theirs(peer)], a.at[mine, block(f)], pk_s, pk_r, expert=peer).start()

        a[mine, block(f)] = xc[mine, :]

    packed = remote(xc.at[seven], rc.at[seven], pk_s, pk_r, expert=next_e)
    plan.compute(["columns", "slots"], "packing", 0.3, pack)
    plan.post(["packing"], "packed", 4.3, lambda: None, packed.wait_recv, 0.0)

    def gather(name, buf, parts, ssem, rsem, start, chunk_work, on_chunk, extra=(), before=()):
        pieces = {}
        for p, (row, rows, kind, zmode, ymode) in enumerate(parts):
            for da, db, sa, sb in spread(kind, zmode, ymode):
                def act(p=p, row=row, rows=rows, kind=kind, da=da, db=db, sa=sa, sb=sb):
                    ref = buf.at[pl.ds(row, rows), block(spot(kind, da, db))]
                    remote(ref, ref, ssem.at[p], rsem.at[p, spot(kind, da, db)], ffn=spot(kind, sa, sb)).start()

                ra, rb = wrap(da - sa, db - sb)

                def wait(p=p, row=row, rows=rows, kind=kind, ra=ra, rb=rb):
                    ref = buf.at[pl.ds(row, rows), block(spot(kind, ra, rb))]
                    remote(ref, ref, ssem.at[p], rsem.at[p, spot(kind, ra, rb)], ffn=next_f).wait_recv()

                held = (name, p, da, db) if (da, db) != (0, 0) else start
                makes = (name, p, ra, rb)
                pieces.setdefault(abs(ra), []).append(makes)
                plan.send([held, *(before if held != start else ())], makes, towards(sa, sb), rows * COL * 2, abs(sa) + abs(sb), act, wait)
        for k in range(5):
            for s in ((1,) if k in (0, 4) else (1, -1)):
                needs = [start, *pieces[k], *extra]
                if k:
                    needs.append((name, "chunk", 0, 1))
                plan.compute(needs, (name, "chunk", k, s), chunk_work,
                             lambda k=k, s=s: on_chunk((z + s * k + NZ) % NZ, k == 0))
        return [(name, "chunk", k, s) for k in range(5) for s in ((1,) if k in (0, 4) else (1, -1))]

    def gather_done(buf, parts, ssem):
        for p, (row, rows, *_) in enumerate(parts):
            ref = buf.at[pl.ds(row, rows), pl.ds(0, COL * (NF - 1))]
            remote(ref, ref, ssem.at[p], lg_r.at[0, 0], ffn=next_f).wait_send()

    plan.bias = U_BIAS
    ups_all = gather("u", ups, WIDE, ug_s, ug_r, loaded(3), 0.0, lambda zi, first: None, (), U_AFTER)

    fins = []
    for g, group in enumerate(GROUPS):
        base, size = group[0][0], sum(part[1] for part in group)
        span = pl.ds(base, size)
        plan.bias = BIAS[g]

        def expert_chunk(zi, first, span=span):
            cols = pl.ds(pl.multiple_of(zi * NY * COL, NY * COL), NY * COL)
            x = a[span, cols]
            left, right = dot(x, wg[cols, :]), dot(x, wu[cols, :])
            if first:
                ga[span, :] = left
                ua[span, :] = right
            else:
                ga[span, :] += left
                ua[span, :] += right

        sub = [ag_s.at[pl.ds(2 * g, 2)], ag_r.at[pl.ds(2 * g, 2)]]
        chunks = gather(("x", g), a, group, *sub, "packed", 0.45 * size / SLOTS + 0.05, expert_chunk,
                        (loaded(4), loaded(5)))

        def hide(span=span):
            gate = ga[span, :]
            hid[span, :] = (gate / (1.0 + jnp.exp(-gate)) * ua[span, :]).astype(BF)

        plan.compute(chunks, ("hid", g), 0.5 * size / SLOTS, hide)
        for k in (4, 3, 2, 1, 0):
            def down(k=k, span=span):
                for s in ((1,) if k in (0, 4) else (1, -1)):
                    zi = (z + s * k + NZ) % NZ
                    cols = pl.ds(pl.multiple_of(zi * NY * COL, NY * COL), NY * COL)
                    pb[span, cols] = dot(hid[span, :], wd[:, cols]).astype(BF)

            plan.compute([("hid", g), loaded(6)], ("pb", g, k), (0.3 if k in (0, 4) else 0.6) * size / SLOTS, down)

        for p, (row, rows, kind, *_) in enumerate(group):
            buf, q = bufs[2 * g + p], 2 * g + p
            slots = {}

            def slot(key, slots=slots):
                return slots.setdefault(key, len(slots))

            def own(da, db, row=row, rows=rows, kind=kind):
                return pb.at[pl.ds(row, rows), block(spot(kind, da, db))]

            def hop(key, needs, parts, sa, sb, buf=buf, q=q, kind=kind, rows=rows, slot=slot):
                to = slot(key)

                def act():
                    refs = [part() for part in parts]
                    if len(refs) > 1:
                        refs[0][...] = add(*[ref[...] for ref in refs])
                    remote(refs[0], buf.at[to], rs_s.at[q], rs_r.at[q, to], ffn=spot(kind, sa, sb)).start()

                def wait():
                    remote(buf.at[to], buf.at[to], rs_s.at[q], rs_r.at[q, to], ffn=next_f).wait_recv()

                plan.send(needs, (q, key), towards(sa, sb), rows * COL * 2, abs(sa) + abs(sb), act, wait,
                          0.02 if len(parts) == 1 else 0.08)

            def here(key, buf=buf, slot=slot):
                return lambda: buf.at[slot(key)]

            def total(makes, needs, parts, out, q=q):
                def act():
                    out()[...] = add(*[part()[...] for part in parts])

                plan.compute(needs, makes, 0.1, act)

            def mid(n, buf=buf):
                return lambda: buf.at[31 + n]

            def mine_at(da, db, own=own):
                return lambda: own(da, db)

            done = ("fin", q)
            final = lambda row=row, rows=rows: fin.at[pl.ds(row, rows), :]
            if kind == 1:
                for da in range(-3, 5):
                    sg, ready = parity(da), ("pb", g, abs(da))
                    hop(("y0", da), [ready], [mine_at(da, 2)], 0, sg)
                    hop(("y2", da), [ready], [mine_at(da, -sg)], 0, -sg)
                    hop(("y1", da), [ready, (q, ("y0", da))], [here(("y0", da)), mine_at(da, sg)], 0, sg)
                    total((q, "sum", da), [ready, (q, ("y1", da)), (q, ("y2", da))],
                          [here(("y1", da)), here(("y2", da)), mine_at(da, 0)], mid(da + 3))
                for s in (1, -1):
                    far = [(q, ("z3", s))] + ([(q, ("z4", s))] if s == 1 else [])
                    if s == 1:
                        hop(("z4", s), [(q, "sum", 4)], [mid(7)], 2, 0)
                    hop(("z3", s), [(q, "sum", 3 * s)], [mid(3 * s + 3)], s, 0)
                    hop(("z2", s), [(q, "sum", 2 * s), *far],
                        [here(("z3", s)), mid(2 * s + 3)] + ([here(("z4", s))] if s == 1 else []), 2 * s, 0)
                    hop(("z1", s), [(q, "sum", s)], [mid(s + 3)], s, 0)
                ends = [("z2", 1), ("z2", -1), ("z1", 1), ("z1", -1)]
                total(done, [(q, "sum", 0)] + [(q, end) for end in ends], [mid(3)] + [here(end) for end in ends], final)
            else:
                for db in range(-1, 3):
                    for s in (1, -1):
                        last = 4 if s == parity(db) else 3
                        for k in range(last, 0, -1):
                            ready = ("pb", g, k)
                            if k == last:
                                hop(("v", db, s, k - 1), [ready], [mine_at(s * k, db)], s, 0)
                            else:
                                hop(("v", db, s, k - 1), [ready, (q, ("v", db, s, k))],
                                    [here(("v", db, s, k)), mine_at(s * k, db)], s, 0)
                    total((q, "sum", db), [("pb", g, 0), (q, ("v", db, 1, 0)), (q, ("v", db, -1, 0))],
                          [mine_at(0, db), here(("v", db, 1, 0)), here(("v", db, -1, 0))], mid(db + 1))
                    if db:
                        hop(("w", db), [(q, "sum", db)], [mid(db + 1)], 0, db)
                total(done, [(q, "sum", 0)] + [(q, ("w", db)) for db in (1, -1, 2)],
                      [mid(1)] + [here(("w", db)) for db in (1, -1, 2)], final)
            fins.append(done)

    plan.bias = 0.0

    def give_back():
        for peer in peers:
            remote(fin.at[theirs(peer)], rc.at[mine], rt_s, rt_r, expert=peer).start()

        rc[mine, :] = fin[mine, :]

    returned = remote(fin.at[seven], rc.at[seven], rt_s, rt_r, expert=next_e)
    plan.post(fins, "back", 4.3, give_back, returned.wait_recv, 0.1)

    def weigh():
        for n in range(NF):
            lf[TF * n:TF * (n + 1), :] = lr[n]
        logits = jnp.transpose(lf[...])[0:NE, :]
        names = lax.broadcasted_iota(jnp.int32, (NE, TOK), 0)
        gap = jnp.sum(logits * (names == routes[0:1, :]).astype(F32), axis=0, keepdims=True)
        gap = gap - jnp.sum(logits * (names == routes[1:2, :]).astype(F32), axis=0, keepdims=True)
        weight0 = 1.0 / (1.0 + jnp.exp(-gap))
        ones[0] = ones[0] * weight0 + ones[1] * (1.0 - weight0)

    plan.compute(["logits", "packed"], "share", 0.5, weigh)

    def combine():
        share = ones[0]
        share_hi = share.astype(BF)
        share_lo = (share - share_hi.astype(F32)).astype(BF)
        back = rc[...]
        mixture = dot(share_hi, back, first_dims) + dot(share_lo, back, first_dims)
        lay[:, block(f)] = (xf[...] + mixture).astype(BF)

    plan.compute(["back", "share"], "layer", 0.3, combine)

    def square():
        own_t = jnp.transpose(lay[:, block(f)].astype(F32)).astype(BF)
        total = jnp.zeros((TOK, COL), F32)
        for n in range(NZ):
            part = dot(own_t, ups[:, n * NY * COL:(n + 1) * NY * COL])
            part = part * part
            total = total + (part[:, 0:128] + part[:, 128:256]) + (part[:, 256:384] + part[:, 384:512])
        ns[...] = jnp.sum(total.reshape(16, 8, COL), axis=0)

        @pl.loop(1, NF)
        def _(j):
            remote(ns, nr.at[f], nm_s, nm_r, ffn=(f + j) % NF).start()

        nr[f] = ns[...]

    norms = remote(nr.at[others], nr.at[others], nm_s, nm_r, ffn=next_f)
    plan.post(["layer", ("early", 0), *ups_all], "norms", 6.0, square, norms.wait_recv, 0.6)

    def scale():
        squared = jnp.sum(jnp.sum(nr[...], axis=0), keepdims=True)
        limit = bound_ref[0]
        factor[...] = jnp.broadcast_to(limit / jnp.maximum(jnp.sqrt(squared), limit), (8, COL))

    plan.compute(["norms"], "factor", 0.2, scale)
    outs = []

    def adapter_chunk(zi, first):
        cols = pl.ds(pl.multiple_of(zi * NY * COL, NY * COL), NY * COL)
        x = lay[:, cols]
        grad = dot(x, ups[:, block(f)], first_dims)
        oc[cols, :] = (grad * factor[0:1, :]).astype(BF)
        out = pltpu.make_async_copy(oc.at[cols, :], clipped_h.at[cols, :], osem.at[1 + len(outs)])
        out.start()
        outs.append(out)
        term = dot(x, adapt[cols, :])
        if first:
            acc[...] = term
        else:
            acc[...] += term

    plan.compute(["layer"], ("early", 0), 0.01, lambda: None)
    gather("l", lay, LAST, lg_s, lg_r, "layer", 0.16, adapter_chunk, ("factor", loaded(7)))
    plan.emit()

    oa[...] = (lay[:, block(f)].astype(F32) + acc[...]).astype(BF)
    first_out = pltpu.make_async_copy(oa, adapted_h, osem.at[0])
    first_out.start()
    columns.wait_send()
    everyone.wait_send()
    packed.wait_send()
    returned.wait_send()
    norms.wait_send()
    gather_done(ups, WIDE, ug_s)
    gather_done(lay, LAST, lg_s)
    gather_done(a, PARTS, ag_s)
    for q, (_, rows, *_) in enumerate(PARTS):
        ref = bufs[q].at[pl.ds(0, NF - 1)]
        remote(ref, ref, rs_s.at[q], rs_r.at[q, 0], ffn=next_f).wait_send()
    first_out.wait()
    for out in outs:
        out.wait()


def pass_on(adapted_h, clipped_h, adapted_out, clipped_out, held, small, sem_in, sem_out):
    steps = [(adapted_h, small, adapted_out)]
    for n in range(4):
        part = pl.ds(n * D // 4, D // 4)
        steps.append((clipped_h.at[part, :], held.at[part, :], clipped_out.at[part, :]))
    ins = [pltpu.make_async_copy(src, mid, sem_in.at[n]) for n, (src, mid, _) in enumerate(steps)]
    outs = [pltpu.make_async_copy(mid, dst, sem_out.at[n]) for n, (_, mid, dst) in enumerate(steps)]
    for copy in ins:
        copy.start()
    for copy, out in zip(ins, outs):
        copy.wait()
        out.start()
    for out in outs:
        out.wait()


def per_device(tokens, routes, router, w_gate, w_up, w_down, adapter, upstream, bound):
    anywhere = pl.BlockSpec(memory_space=pl.ANY)
    vmem = pltpu.VMEM
    dma = pltpu.SemaphoreType.DMA
    adapted, clipped = pl.pallas_call(
        kernel,
        out_shape=(
            jax.ShapeDtypeStruct((TOK, COL), BF),
            jax.ShapeDtypeStruct((D, COL), BF),
        ),
        in_specs=[anywhere] * 8 + [pl.BlockSpec(memory_space=pltpu.SMEM)],
        out_specs=(anywhere, anywhere),
        scratch_shapes=[
            vmem((TF, D), BF), vmem((2, TOK), jnp.int32), vmem((NE, D), BF),
            vmem((D, FD), BF), vmem((D, FD), BF), vmem((FD, D), BF), vmem((D, COL), BF),
            vmem((NF, TF, COL), BF), vmem((NF, TF, COL), F32), vmem((TF, COL), F32),
            vmem((TOK, COL), F32), vmem((TOK, COL), F32),
            vmem((SLOTS, COL), BF), vmem((SLOTS, D), BF),
            vmem((SLOTS, FD), F32), vmem((SLOTS, FD), F32), vmem((SLOTS, FD), BF), vmem((SLOTS, D), BF),
            *[vmem((39, part[1], COL), BF) for part in PARTS],
            vmem((SLOTS, COL), BF), vmem((SLOTS, COL), BF),
            vmem((TOK, D), BF), vmem((TOK, D), BF), vmem((TOK, COL), F32), vmem((2, SLOTS, TOK), F32),
            vmem((8, COL), F32), vmem((NF, 8, COL), F32), vmem((8, COL), F32),
            vmem((TOK, COL), BF), vmem((D, COL), BF),
            dma((8,)), dma((9,)), dma, dma, dma, dma, dma, dma, dma, dma, dma, dma,
            dma((len(PARTS),)), dma((len(PARTS), NF)), dma((len(PARTS),)), dma((len(PARTS), NF - 1)),
            dma((2,)), dma((2, NF)), dma((2,)), dma((2, NF)),
        ],
        compiler_params=pltpu.CompilerParams(
            collective_id=0, has_side_effects=True, vmem_limit_bytes=60 * 1024 * 1024
        ),
    )(
        tokens[0], jnp.transpose(routes[0]), jnp.transpose(router), w_gate[0], w_up[0], w_down[0],
        adapter[0], upstream[0], bound,
    )
    shapes = (jax.ShapeDtypeStruct((TOK, COL), BF), jax.ShapeDtypeStruct((D, COL), BF))
    adapted, clipped = pl.pallas_call(
        pass_on,
        out_shape=shapes,
        in_specs=[anywhere] * 2,
        out_specs=(anywhere, anywhere),
        scratch_shapes=[vmem((D, COL), BF), vmem((TOK, COL), BF), dma((5,)), dma((5,))],
    )(adapted, clipped)
    return adapted[None], clipped[None]


def solution(mesh):
    placed = (
        P("expert", "ffn", None),
        P("expert", None, None),
        P(),
        P("expert", None, "ffn"),
        P("expert", None, "ffn"),
        P("expert", "ffn", None),
        P("expert", None, "ffn"),
        P("expert", None, "ffn"),
        P("expert"),
    )
    return jax.shard_map(
        per_device,
        mesh=mesh,
        in_specs=placed,
        out_specs=(P("expert", None, "ffn"), P("expert", None, "ffn")),
        check_vma=False,
    )
```

```python
import jax
import jax.numpy as jnp
from jax import lax
from jax.experimental import pallas as pl
from jax.experimental.pallas import tpu as pltpu
from jax.sharding import PartitionSpec as P

MESH = pl.DeviceIdType.MESH
BF = jnp.bfloat16
F32 = jnp.float32
NZ, NY = 8, 4
NF = NZ * NY
NE = 8
CAP = 48
TOK = 128
TF = TOK // NF
D = 4096
FD = 384
COL = 128
SLOTS = NE * CAP
GROUPS = (((0, 240, 1, 1, 4), (240, 144, 2, 0, 0)),)
WIDE = ((0, 80, 1, 1, 5), (80, 48, 2, 1, 0))
LAST = ((0, 80, 1, 1, 1), (80, 48, 2, 1, 0))
PARTS = tuple(part for group in GROUPS for part in group)
RATE = {("z", True): 50e3, ("z", False): 43e3, ("y", True): 48.5e3, ("y", False): 44.5e3}
FIRST_HOP, NEXT_HOP, LEAD = 3.0, 0.75, 0.8
BIAS, U_BIAS = (0.0, 0.0), 0.0
U_AFTER = ()


def dot(a, b, dims=(((1,), (0,)), ((), ()))):
    return lax.dot_general(a, b, dims, preferred_element_type=F32)


def block(index):
    return pl.ds(pl.multiple_of(index * COL, COL), COL)


def add(*parts):
    total = parts[0].astype(F32)
    for part in parts[1:]:
        total = total + part.astype(F32)
    return total.astype(BF)


def parity(v):
    return 1 if v % 2 == 0 else -1


def spread(kind, zmode, ymode):
    out = []

    def along(b, s0):
        for s in (1, -1):
            out.append((0, b, s, 0))
            if zmode == 2:
                out.extend(((0, b, 2 * s, 0), (0, b, 3 * s, 0)))
                if s == s0:
                    out.append((0, b, 4 * s, 0))
            elif zmode == 1:
                out.extend(((0, b, 2 * s, 0), (-2 * s, b, s, 0)))
                if s == s0:
                    out.append((-2 * s, b, 2 * s, 0))
            else:
                out.extend(((-s, b, s, 0), (-2 * s, b, s, 0)))
                if s == s0:
                    out.append((-3 * s, b, s, 0))

    if kind == 1:
        along(0, 1)
        for a in range(-3, 5):
            sg = parity(a)
            out.extend(((a, 0, 0, 1), (a, 0, 0, -1), (a, 0, 0, 2 * sg) if abs(a) >= ymode else (a, -sg, 0, sg)))
    else:
        out.extend(((0, 0, 0, 1), (0, 0, 0, -1), (0, 0, 0, 2)))
        for b in range(-1, 3):
            along(b, parity(b))
    return out


def wrap(a, b):
    return (a + 3) % 8 - 3, (b + 1) % 4 - 1


class Plan:
    def __init__(self):
        self.nodes = []
        self.waits = {}
        self.given = {}
        self.bias = 0.0

    def send(self, needs, makes, link, size, hops, act, wait, work=0.02):
        self.nodes.append(dict(needs=needs, makes=makes, link=link, cost=size / RATE[link], hops=hops, act=act, work=work, bias=self.bias))
        self.waits[makes] = wait

    def post(self, needs, makes, delay, act, wait, work=0.1):
        self.nodes.append(dict(needs=needs, makes=makes, link=None, delay=delay, act=act, work=work, bias=self.bias))
        self.waits[makes] = wait

    def compute(self, needs, makes, work, act):
        self.nodes.append(dict(needs=needs, makes=makes, link=None, delay=0.0, act=act, work=work, bias=self.bias))

    def order(self):
        users = {}
        for node in self.nodes:
            for need in node["needs"]:
                users.setdefault(need, []).append(node)
        length = {}

        def path(node):
            key = id(node)
            if key not in length:
                if node["link"] is None:
                    own = node["work"] + node["delay"]
                else:
                    own = node["work"] + node["cost"] * node["hops"] + FIRST_HOP + NEXT_HOP * (node["hops"] - 1)
                length[key] = own + max([path(user) for user in users.get(node["makes"], ())] or [0.0])
            return length[key]

        for node in self.nodes:
            path(node)
        known, free, core, busy, out = dict(self.given), {}, 0.0, (0.0, 0.0), []
        pending = list(self.nodes)
        while pending:
            best = None
            for at, node in enumerate(pending):
                if any(need not in known for need in node["needs"]):
                    continue
                ready = max([known[need] for need in node["needs"]] or [0.0])
                if node["link"] is None:
                    start = max(ready, core)
                else:
                    if busy[0] < ready < busy[1]:
                        ready = busy[1]
                    start = max(ready, free.get(node["link"], 0.0))
                key = (round(start, 2), node["link"] is None and node["work"] > 0.15, -length[id(node)] - node["bias"], at)
                if best is None or key < best[0]:
                    best = (key, node, ready, start)
            _, node, ready, start = best
            pending.remove(node)
            if node["link"] is None:
                core = start + node["work"]
                busy = (start, core)
                known[node["makes"]] = core + node["delay"]
                out.append((start, len(out), node))
            else:
                free[node["link"]] = start + node["cost"] * node["hops"]
                known[node["makes"]] = start + node["work"] + node["cost"] + FIRST_HOP + NEXT_HOP * (node["hops"] - 1)
                out.append((max(ready, start - LEAD), len(out), node))
        return [node for _, _, node in sorted(out, key=lambda item: item[:2])], max(known.values())

    def emit(self):
        order, _ = self.order()
        waited = set()
        for node in order:
            for need in node["needs"]:
                if need in self.waits and need not in waited:
                    waited.add(need)
                    self.waits[need]()
            node["act"]()
        for need, wait in self.waits.items():
            if need not in waited:
                wait()


def kernel(
    tok_h, routes_h, router_h, gate_h, up_h, down_h, adapt_h, upstr_h, bound_ref,
    adapted_h, clipped_h,
    tok, routes, router, wg, wu, wd, adapt, xr, lr, ls, xf, lf, xc, a, ga, ua, hid, pb, *rest,
):
    bufs, rest = rest[:len(PARTS)], rest[len(PARTS):]
    (fin, rc, lay, ups, acc, ones, ns, nr, factor, oa, oc,
     lsem, osem, a2a_s, a2a_r, log_s, log_r, pk_s, pk_r, rt_s, rt_r, nm_s, nm_r,
     ag_s, ag_r, rs_s, rs_r, lg_s, lg_r, ug_s, ug_r) = rest
    e = lax.axis_index("expert")
    f = lax.axis_index("ffn")
    z, y = f // NY, f % NY
    core = e % 2
    turn = 1 - 2 * core
    turn_y = {1: turn, 2: 1}
    first_dims = (((0,), (0,)), ((), ()))

    def spot(kind, da, db):
        zi = (z + turn * da + 2 * NZ) % NZ
        yi = (y + turn_y[kind] * db + 2 * NY) % NY
        return zi * NY + yi

    def remote(src, dst, ss, rs, **where):
        return pltpu.make_async_remote_copy(
            src_ref=src, dst_ref=dst, send_sem=ss, recv_sem=rs,
            device_id=where, device_id_type=MESH,
        )

    def towards(da, db):
        return ("z", da > 0) if da else ("y", db > 0)

    loads = [
        pltpu.make_async_copy(src, dst, lsem.at[n])
        for n, (src, dst) in enumerate(
            ((tok_h, tok), (routes_h, routes), (router_h, router), (upstr_h, ups.at[:, block(f)]),
             (gate_h, wg), (up_h, wu), (down_h, wd), (adapt_h, adapt))
        )
    ]
    for load in loads:
        load.start()

    barrier = pltpu.get_barrier_semaphore()

    @pl.loop(1, NF)
    def _(j):
        pl.semaphore_signal(barrier, inc=1, device_id={"ffn": (f + j) % NF}, device_id_type=MESH)

    @pl.loop(1, NE)
    def _(j):
        pl.semaphore_signal(barrier, inc=1, device_id={"expert": (e + j) % NE}, device_id_type=MESH)

    loads[0].wait()
    pl.semaphore_wait(barrier, NF - 1 + NE - 1)

    plan = Plan()
    others = pl.ds(0, NF - 1)
    seven = pl.ds(0, CAP * (NE - 1))
    mine = pl.ds(pl.multiple_of(e * CAP, CAP), CAP)
    next_f, next_e = (f + 1) % NF, (e + 1) % NE

    peers = [(e // 2 + chip) % (NE // 2) * 2 + other for chip in (2, 1, 3) for other in (0, 1)] + [e + turn]

    def theirs(peer):
        return pl.ds(pl.multiple_of(peer * CAP, CAP), CAP)

    def loaded(n):
        plan.waits["load", n] = loads[n].wait
        plan.given["load", n] = 0.0
        return "load", n

    def to_columns():
        @pl.loop(1, NF)
        def _(j):
            peer = (f + j) % NF
            remote(tok.at[:, block(peer)], xr.at[f], a2a_s, a2a_r, ffn=peer).start()

        xr[f] = tok[:, block(f)]

    columns = remote(xr.at[others], xr.at[others], a2a_s, a2a_r, ffn=next_f)
    plan.post([], "columns", 4.6, to_columns, columns.wait_recv, 0.2)

    def own_logits():
        loads[2].wait()
        ls[...] = jnp.zeros_like(ls)
        ls[:, 0:NE] = dot(tok[...], router[...], (((1,), (1,)), ((), ())))

        @pl.loop(1, NF)
        def _(j):
            remote(ls, lr.at[f], log_s, log_r, ffn=(f + j) % NF).start()

        lr[f] = ls[...]

    everyone = remote(lr.at[others], lr.at[others], log_s, log_r, ffn=next_f)
    plan.post([], "logits", 6.0, own_logits, everyone.wait_recv, 0.55)

    def own_slots():
        loads[1].wait()
        r0, r1 = routes[0:1, :], routes[1:2, :]
        names = lax.broadcasted_iota(jnp.int32, (NE, TOK), 0)
        h0 = (names == r0).astype(F32)
        h1 = (names == r1).astype(F32)
        early = lax.broadcasted_iota(jnp.int32, (TOK, TOK), 0) < lax.broadcasted_iota(jnp.int32, (TOK, TOK), 1)
        before = dot((h0 + h1).astype(BF), early.astype(F32).astype(BF))
        slot0 = jnp.sum(before * h0, axis=0, keepdims=True).astype(jnp.int32) + r0 * CAP
        slot1 = jnp.sum(before * h1, axis=0, keepdims=True).astype(jnp.int32) + r1 * CAP
        places = lax.broadcasted_iota(jnp.int32, (SLOTS, TOK), 0)
        ones[0] = (places == slot0).astype(F32)
        ones[1] = (places == slot1).astype(F32)

    plan.compute([], "slots", 0.2, own_slots)

    def pack():
        for n in range(NF):
            xf[TF * n:TF * (n + 1), :] = xr[n].astype(F32)
        xc[...] = dot((ones[0] + ones[1]).astype(BF), xf[...].astype(BF)).astype(BF)

        for peer in peers:
            remote(xc.at[theirs(peer)], a.at[mine, block(f)], pk_s, pk_r, expert=peer).start()

        a[mine, block(f)] = xc[mine, :]

    packed = remote(xc.at[seven], rc.at[seven], pk_s, pk_r, expert=next_e)
    plan.compute(["columns", "slots"], "packing", 0.3, pack)
    plan.post(["packing"], "packed", 4.3, lambda: None, packed.wait_recv, 0.0)

    def gather(name, buf, parts, ssem, rsem, start, chunk_work, on_chunk, extra=(), before=()):
        pieces = {}
        for p, (row, rows, kind, zmode, ymode) in enumerate(parts):
            for da, db, sa, sb in spread(kind, zmode, ymode):
                def act(p=p, row=row, rows=rows, kind=kind, da=da, db=db, sa=sa, sb=sb):
                    ref = buf.at[pl.ds(row, rows), block(spot(kind, da, db))]
                    remote(ref, ref, ssem.at[p], rsem.at[p, spot(kind, da, db)], ffn=spot(kind, sa, sb)).start()

                ra, rb = wrap(da - sa, db - sb)

                def wait(p=p, row=row, rows=rows, kind=kind, ra=ra, rb=rb):
                    ref = buf.at[pl.ds(row, rows), block(spot(kind, ra, rb))]
                    remote(ref, ref, ssem.at[p], rsem.at[p, spot(kind, ra, rb)], ffn=next_f).wait_recv()

                held = (name, p, da, db) if (da, db) != (0, 0) else start
                makes = (name, p, ra, rb)
                pieces.setdefault(abs(ra), []).append(makes)
                plan.send([held, *(before if held != start else ())], makes, towards(sa, sb), rows * COL * 2, abs(sa) + abs(sb), act, wait)
        for k in range(5):
            for s in ((1,) if k in (0, 4) else (1, -1)):
                needs = [start, *pieces[k], *extra]
                if k:
                    needs.append((name, "chunk", 0, 1))
                plan.compute(needs, (name, "chunk", k, s), chunk_work,
                             lambda k=k, s=s: on_chunk((z + s * k + NZ) % NZ, k == 0))
        return [(name, "chunk", k, s) for k in range(5) for s in ((1,) if k in (0, 4) else (1, -1))]

    def gather_done(buf, parts, ssem):
        for p, (row, rows, *_) in enumerate(parts):
            ref = buf.at[pl.ds(row, rows), pl.ds(0, COL * (NF - 1))]
            remote(ref, ref, ssem.at[p], lg_r.at[0, 0], ffn=next_f).wait_send()

    plan.bias = U_BIAS
    ups_all = gather("u", ups, WIDE, ug_s, ug_r, loaded(3), 0.0, lambda zi, first: None, (), U_AFTER)

    fins = []
    for g, group in enumerate(GROUPS):
        base, size = group[0][0], sum(part[1] for part in group)
        span = pl.ds(base, size)
        plan.bias = BIAS[g]

        def expert_chunk(zi, first, span=span):
            cols = pl.ds(pl.multiple_of(zi * NY * COL, NY * COL), NY * COL)
            x = a[span, cols]
            left, right = dot(x, wg[cols, :]), dot(x, wu[cols, :])
            if first:
                ga[span, :] = left
                ua[span, :] = right
            else:
                ga[span, :] += left
                ua[span, :] += right

        sub = [ag_s.at[pl.ds(2 * g, 2)], ag_r.at[pl.ds(2 * g, 2)]]
        chunks = gather(("x", g), a, group, *sub, "packed", 0.45 * size / SLOTS + 0.05, expert_chunk,
                        (loaded(4), loaded(5)))

        def hide(span=span):
            gate = ga[span, :]
            hid[span, :] = (gate / (1.0 + jnp.exp(-gate)) * ua[span, :]).astype(BF)

        plan.compute(chunks, ("hid", g), 0.5 * size / SLOTS, hide)
        for k in (4, 3, 2, 1, 0):
            def down(k=k, span=span):
                for s in ((1,) if k in (0, 4) else (1, -1)):
                    zi = (z + s * k + NZ) % NZ
                    cols = pl.ds(pl.multiple_of(zi * NY * COL, NY * COL), NY * COL)
                    pb[span, cols] = dot(hid[span, :], wd[:, cols]).astype(BF)

            plan.compute([("hid", g), loaded(6)], ("pb", g, k), (0.3 if k in (0, 4) else 0.6) * size / SLOTS, down)

        for p, (row, rows, kind, *_) in enumerate(group):
            buf, q = bufs[2 * g + p], 2 * g + p
            slots = {}

            def slot(key, slots=slots):
                return slots.setdefault(key, len(slots))

            def own(da, db, row=row, rows=rows, kind=kind):
                return pb.at[pl.ds(row, rows), block(spot(kind, da, db))]

            def hop(key, needs, parts, sa, sb, buf=buf, q=q, kind=kind, rows=rows, slot=slot):
                to = slot(key)

                def act():
                    refs = [part() for part in parts]
                    if len(refs) > 1:
                        refs[0][...] = add(*[ref[...] for ref in refs])
                    remote(refs[0], buf.at[to], rs_s.at[q], rs_r.at[q, to], ffn=spot(kind, sa, sb)).start()

                def wait():
                    remote(buf.at[to], buf.at[to], rs_s.at[q], rs_r.at[q, to], ffn=next_f).wait_recv()

                plan.send(needs, (q, key), towards(sa, sb), rows * COL * 2, abs(sa) + abs(sb), act, wait,
                          0.02 if len(parts) == 1 else 0.08)

            def here(key, buf=buf, slot=slot):
                return lambda: buf.at[slot(key)]

            def total(makes, needs, parts, out, q=q):
                def act():
                    out()[...] = add(*[part()[...] for part in parts])

                plan.compute(needs, makes, 0.1, act)

            def mid(n, buf=buf):
                return lambda: buf.at[31 + n]

            def mine_at(da, db, own=own):
                return lambda: own(da, db)

            done = ("fin", q)
            final = lambda row=row, rows=rows: fin.at[pl.ds(row, rows), :]
            if kind == 1:
                for da in range(-3, 5):
                    sg, ready = parity(da), ("pb", g, abs(da))
                    hop(("y0", da), [ready], [mine_at(da, 2)], 0, sg)
                    hop(("y2", da), [ready], [mine_at(da, -sg)], 0, -sg)
                    hop(("y1", da), [ready, (q, ("y0", da))], [here(("y0", da)), mine_at(da, sg)], 0, sg)
                    total((q, "sum", da), [ready, (q, ("y1", da)), (q, ("y2", da))],
                          [here(("y1", da)), here(("y2", da)), mine_at(da, 0)], mid(da + 3))
                for s in (1, -1):
                    far = [(q, ("z3", s))] + ([(q, ("z4", s))] if s == 1 else [])
                    if s == 1:
                        hop(("z4", s), [(q, "sum", 4)], [mid(7)], 2, 0)
                    hop(("z3", s), [(q, "sum", 3 * s)], [mid(3 * s + 3)], s, 0)
                    hop(("z2", s), [(q, "sum", 2 * s), *far],
                        [here(("z3", s)), mid(2 * s + 3)] + ([here(("z4", s))] if s == 1 else []), 2 * s, 0)
                    hop(("z1", s), [(q, "sum", s)], [mid(s + 3)], s, 0)
                ends = [("z2", 1), ("z2", -1), ("z1", 1), ("z1", -1)]
                total(done, [(q, "sum", 0)] + [(q, end) for end in ends], [mid(3)] + [here(end) for end in ends], final)
            else:
                for db in range(-1, 3):
                    for s in (1, -1):
                        last = 4 if s == parity(db) else 3
                        for k in range(last, 0, -1):
                            ready = ("pb", g, k)
                            if k == last:
                                hop(("v", db, s, k - 1), [ready], [mine_at(s * k, db)], s, 0)
                            else:
                                hop(("v", db, s, k - 1), [ready, (q, ("v", db, s, k))],
                                    [here(("v", db, s, k)), mine_at(s * k, db)], s, 0)
                    total((q, "sum", db), [("pb", g, 0), (q, ("v", db, 1, 0)), (q, ("v", db, -1, 0))],
                          [mine_at(0, db), here(("v", db, 1, 0)), here(("v", db, -1, 0))], mid(db + 1))
                    if db:
                        hop(("w", db), [(q, "sum", db)], [mid(db + 1)], 0, db)
                total(done, [(q, "sum", 0)] + [(q, ("w", db)) for db in (1, -1, 2)],
                      [mid(1)] + [here(("w", db)) for db in (1, -1, 2)], final)
            fins.append(done)

    plan.bias = 0.0

    def give_back():
        for peer in peers:
            remote(fin.at[theirs(peer)], rc.at[mine], rt_s, rt_r, expert=peer).start()

        rc[mine, :] = fin[mine, :]

    returned = remote(fin.at[seven], rc.at[seven], rt_s, rt_r, expert=next_e)
    plan.post(fins, "back", 4.3, give_back, returned.wait_recv, 0.1)

    def weigh():
        for n in range(NF):
            lf[TF * n:TF * (n + 1), :] = lr[n]
        logits = jnp.transpose(lf[...])[0:NE, :]
        names = lax.broadcasted_iota(jnp.int32, (NE, TOK), 0)
        gap = jnp.sum(logits * (names == routes[0:1, :]).astype(F32), axis=0, keepdims=True)
        gap = gap - jnp.sum(logits * (names == routes[1:2, :]).astype(F32), axis=0, keepdims=True)
        weight0 = 1.0 / (1.0 + jnp.exp(-gap))
        ones[0] = ones[0] * weight0 + ones[1] * (1.0 - weight0)

    plan.compute(["logits", "packed"], "share", 0.5, weigh)

    def combine():
        share = ones[0]
        share_hi = share.astype(BF)
        share_lo = (share - share_hi.astype(F32)).astype(BF)
        back = rc[...]
        mixture = dot(share_hi, back, first_dims) + dot(share_lo, back, first_dims)
        lay[:, block(f)] = (xf[...] + mixture).astype(BF)

    plan.compute(["back", "share"], "layer", 0.3, combine)

    def square():
        own_t = jnp.transpose(lay[:, block(f)].astype(F32)).astype(BF)
        total = jnp.zeros((TOK, COL), F32)
        for n in range(NZ):
            part = dot(own_t, ups[:, n * NY * COL:(n + 1) * NY * COL])
            part = part * part
            total = total + (part[:, 0:128] + part[:, 128:256]) + (part[:, 256:384] + part[:, 384:512])
        ns[...] = jnp.sum(total.reshape(16, 8, COL), axis=0)

        @pl.loop(1, NF)
        def _(j):
            remote(ns, nr.at[f], nm_s, nm_r, ffn=(f + j) % NF).start()

        nr[f] = ns[...]

    norms = remote(nr.at[others], nr.at[others], nm_s, nm_r, ffn=next_f)
    plan.post(["layer", ("early", 0), *ups_all], "norms", 6.0, square, norms.wait_recv, 0.6)

    def scale():
        squared = jnp.sum(jnp.sum(nr[...], axis=0), keepdims=True)
        limit = bound_ref[0]
        factor[...] = jnp.broadcast_to(limit / jnp.maximum(jnp.sqrt(squared), limit), (8, COL))

    plan.compute(["norms"], "factor", 0.2, scale)
    outs = []

    def adapter_chunk(zi, first):
        cols = pl.ds(pl.multiple_of(zi * NY * COL, NY * COL), NY * COL)
        x = lay[:, cols]
        grad = dot(x, ups[:, block(f)], first_dims)
        oc[cols, :] = (grad * factor[0:1, :]).astype(BF)
        out = pltpu.make_async_copy(oc.at[cols, :], clipped_h.at[cols, :], osem.at[1 + len(outs)])
        out.start()
        outs.append(out)
        term = dot(x, adapt[cols, :])
        if first:
            acc[...] = term
        else:
            acc[...] += term

    plan.compute(["layer"], ("early", 0), 0.01, lambda: None)
    gather("l", lay, LAST, lg_s, lg_r, "layer", 0.16, adapter_chunk, ("factor", loaded(7)))
    plan.emit()

    oa[...] = (lay[:, block(f)].astype(F32) + acc[...]).astype(BF)
    first_out = pltpu.make_async_copy(oa, adapted_h, osem.at[0])
    first_out.start()
    columns.wait_send()
    everyone.wait_send()
    packed.wait_send()
    returned.wait_send()
    norms.wait_send()
    gather_done(ups, WIDE, ug_s)
    gather_done(lay, LAST, lg_s)
    gather_done(a, PARTS, ag_s)
    for q, (_, rows, *_) in enumerate(PARTS):
        ref = bufs[q].at[pl.ds(0, NF - 1)]
        remote(ref, ref, rs_s.at[q], rs_r.at[q, 0], ffn=next_f).wait_send()
    first_out.wait()
    for out in outs:
        out.wait()


def pass_on(adapted_h, clipped_h, adapted_out, clipped_out, held, small, sem_in, sem_out):
    steps = [(adapted_h, small, adapted_out)]
    for n in range(4):
        part = pl.ds(n * D // 4, D // 4)
        steps.append((clipped_h.at[part, :], held.at[part, :], clipped_out.at[part, :]))
    ins = [pltpu.make_async_copy(src, mid, sem_in.at[n]) for n, (src, mid, _) in enumerate(steps)]
    outs = [pltpu.make_async_copy(mid, dst, sem_out.at[n]) for n, (_, mid, dst) in enumerate(steps)]
    for copy in ins:
        copy.start()
    for copy, out in zip(ins, outs):
        copy.wait()
        out.start()
    for out in outs:
        out.wait()


def per_device(tokens, routes, router, w_gate, w_up, w_down, adapter, upstream, bound):
    anywhere = pl.BlockSpec(memory_space=pl.ANY)
    vmem = pltpu.VMEM
    dma = pltpu.SemaphoreType.DMA
    adapted, clipped = pl.pallas_call(
        kernel,
        out_shape=(
            jax.ShapeDtypeStruct((TOK, COL), BF),
            jax.ShapeDtypeStruct((D, COL), BF),
        ),
        in_specs=[anywhere] * 8 + [pl.BlockSpec(memory_space=pltpu.SMEM)],
        out_specs=(anywhere, anywhere),
        scratch_shapes=[
            vmem((TF, D), BF), vmem((2, TOK), jnp.int32), vmem((NE, D), BF),
            vmem((D, FD), BF), vmem((D, FD), BF), vmem((FD, D), BF), vmem((D, COL), BF),
            vmem((NF, TF, COL), BF), vmem((NF, TF, COL), F32), vmem((TF, COL), F32),
            vmem((TOK, COL), F32), vmem((TOK, COL), F32),
            vmem((SLOTS, COL), BF), vmem((SLOTS, D), BF),
            vmem((SLOTS, FD), F32), vmem((SLOTS, FD), F32), vmem((SLOTS, FD), BF), vmem((SLOTS, D), BF),
            *[vmem((39, part[1], COL), BF) for part in PARTS],
            vmem((SLOTS, COL), BF), vmem((SLOTS, COL), BF),
            vmem((TOK, D), BF), vmem((TOK, D), BF), vmem((TOK, COL), F32), vmem((2, SLOTS, TOK), F32),
            vmem((8, COL), F32), vmem((NF, 8, COL), F32), vmem((8, COL), F32),
            vmem((TOK, COL), BF), vmem((D, COL), BF),
            dma((8,)), dma((9,)), dma, dma, dma, dma, dma, dma, dma, dma, dma, dma,
            dma((len(PARTS),)), dma((len(PARTS), NF)), dma((len(PARTS),)), dma((len(PARTS), NF - 1)),
            dma((2,)), dma((2, NF)), dma((2,)), dma((2, NF)),
        ],
        compiler_params=pltpu.CompilerParams(
            collective_id=0, has_side_effects=True, vmem_limit_bytes=60 * 1024 * 1024
        ),
    )(
        tokens[0], jnp.transpose(routes[0]), jnp.transpose(router), w_gate[0], w_up[0], w_down[0],
        adapter[0], upstream[0], bound,
    )
    shapes = (jax.ShapeDtypeStruct((TOK, COL), BF), jax.ShapeDtypeStruct((D, COL), BF))
    adapted, clipped = pl.pallas_call(
        pass_on,
        out_shape=shapes,
        in_specs=[anywhere] * 2,
        out_specs=(anywhere, anywhere),
        scratch_shapes=[vmem((D, COL), BF), vmem((TOK, COL), BF), dma((5,)), dma((5,))],
    )(adapted, clipped)
    return adapted[None], clipped[None]


def solution(mesh):
    placed = (
        P("expert", "ffn", None),
        P("expert", None, None),
        P(),
        P("expert", None, "ffn"),
        P("expert", None, "ffn"),
        P("expert", "ffn", None),
        P("expert", None, "ffn"),
        P("expert", None, "ffn"),
        P("expert"),
    )
    return jax.shard_map(
        per_device,
        mesh=mesh,
        in_specs=placed,
        out_specs=(P("expert", None, "ffn"), P("expert", None, "ffn")),
        check_vma=False,
    )
```
